32 devices in a mesh: gx: 4 (over z), gy: 2 (over y), gz: 4 (over x, core).
Axes of the slice: x: 2, y: 2, z: 4, core: 2. Of those that a mesh axis runs over, the one named last changes fastest.
Arguments:
- state: float32 [9, 64, 32, 512], P(None, 'gx', 'gy', 'gz'), may hold values from 0 to 1
- mobility: float32 [8], replicated, may hold values from 0.5 to 2
- seeds: int32 [2, 2, 64, 32], replicated, may hold values from 0 to 8
- frame_shifts: int32 [2], replicated, may hold values from 0 to 2, as said below
Outputs:
- state_out: float32 [9, 64, 32, 512], P(None, 'gx', 'gy', 'gz')
The draws below stay inside these ranges and needn't reach their ends.
Inputs may be any that keep to these rules, and one draw needn't show every extreme that they name: A value of 8 seeds no grain in that cell. `frame_shifts`: the frame advances 2 planes in at least one step and stays in place in at least one other.
All inputs are finite; a program needn't handle non-finite values.
Results may differ from the reference program's by a relative error of at most 0.0001.
Values sent between devices are 32-bit elements; how exact they have to be, the bound alone decides.
No kernel may reach another device: no remote copies, remote signals or barrier semaphores. Data moves between devices by JAX's collectives and lax.ppermute only.
A program may use at most 64 MiB of HBM per device.

```python
import math
import jax
import jax.numpy as jnp
from jax import lax

GRAINS = 8
STEPS = 2
SHIFT_MAX = 2
NX = 64
NY = 32
NZ = 512


def draw_frame_shifts(key, part):
    counts = jax.random.randint(key, (STEPS,), 0, SHIFT_MAX + 1, dtype=jnp.int32)
    which = jax.random.randint(jax.random.fold_in(key, 7), (), 0, STEPS, dtype=jnp.int32)
    offset = jax.random.randint(jax.random.fold_in(key, 11), (), 0, STEPS - 1, dtype=jnp.int32)
    other = (which + 1 + offset) % STEPS
    steps_all = jnp.arange(STEPS, dtype=jnp.int32)
    counts = jnp.where(steps_all == other, 0, counts)
    return jnp.where(steps_all == which, SHIFT_MAX, counts).astype(jnp.int32)


def plant(array, stream_key, least, largest):
    longest = array.shape.index(max(array.shape))
    spots = []
    for shift in (0, 1):
        where = [jax.random.randint(jax.random.fold_in(stream_key, axis), (), 0, length) for axis, length in enumerate(array.shape)]
        where[longest] = (where[longest] + shift) % array.shape[longest]
        spots.append(tuple(where))
    return array.at[spots[0]].set(least).at[spots[1]].set(largest)


def level_of(own_key, dims, cuts, smallest, top_value):
    loudness = 1.0
    for dim, parts in cuts:
        draws = jax.random.uniform(jax.random.fold_in(jax.random.fold_in(own_key, 6), dim), (parts,), jnp.float32, smallest / len(cuts), top_value / len(cuts))
        loudness = loudness * jnp.repeat(jnp.exp(draws), dims[dim] // parts).reshape((-1,) + (1,) * (len(dims) - 1 - dim))
    return loudness


def setup_inputs(seed: int = 0) -> dict:
    keys = jax.random.split(jax.random.key(seed), 5)
    state = jnp.clip(1.0 * jax.random.uniform(keys[0], (GRAINS + 1, NX, NY, NZ), jnp.float32) ** level_of(keys[0], (GRAINS + 1, NX, NY, NZ), ((1, 4), (2, 2), (3, 4)), -0.2, 0.2), 0.0, 1.0)
    mobility = jnp.clip(jnp.exp(jax.random.uniform(keys[1], (GRAINS,), jnp.float32, math.log(0.5), math.log(2.0))), 0.5, 2.0)
    seeds = plant(jax.random.randint(keys[2], (STEPS, SHIFT_MAX, NX, NY), 0, GRAINS + 1), jax.random.fold_in(keys[2], 1), 0, GRAINS).astype(jnp.int32)
    frame_shifts = draw_frame_shifts(jax.random.fold_in(keys[4], 71), 0)
    return dict(state=state, mobility=mobility, seeds=seeds, frame_shifts=frame_shifts)


step_rate = 0.1
stiffness = 0.7
coupling = 0.5
diffusion = 0.14
rejection = 0.5
nucleus = 0.3
melt_solute = 1.0


def laplace(field):
    padded = jnp.pad(field, ((1, 1), (1, 1), (0, 0)), mode="wrap")
    padded = jnp.pad(padded, ((0, 0), (0, 0), (1, 1)))
    center = padded[1:-1, 1:-1, 1:-1]
    beside = padded[:-2, 1:-1, 1:-1] + padded[2:, 1:-1, 1:-1] + padded[1:-1, :-2, 1:-1] + padded[1:-1, 2:, 1:-1]
    beside = beside + padded[1:-1, 1:-1, :-2] + padded[1:-1, 1:-1, 2:]
    return beside - 6.0 * center


def advance(moved, mobility):
    phases = moved[:GRAINS]
    solute = moved[GRAINS]
    squares = jnp.sum(phases * phases, axis=0)
    zpos = jnp.arange(NZ, dtype=jnp.float32)
    theta = 1.0 - 2.0 * (zpos + 0.5) / NZ
    alpha = theta - coupling * solute

    def single(item):
        phase, speed = item
        drive = -alpha * phase + phase * phase * phase + phase * (squares - phase * phase)
        return phase + step_rate * speed * (stiffness * laplace(phase) - drive)

    fresh = lax.map(single, (phases, mobility))
    squares_new = jnp.sum(fresh * fresh, axis=0)
    solute_new = solute + diffusion * laplace(solute) - rejection * solute * (squares_new - squares)
    return jnp.concatenate([fresh, solute_new[None]], axis=0)


def reference(state, mobility, seeds, frame_shifts):
    field = state
    grains = jnp.arange(GRAINS, dtype=jnp.int32)
    for step in range(STEPS):
        count = frame_shifts[step].astype(jnp.int32)
        marks = jnp.transpose(seeds[step], (1, 2, 0))
        nuclei = nucleus * (marks[None] == grains[:, None, None, None]).astype(jnp.float32)
        melt = jnp.full((1, NX, NY, SHIFT_MAX), melt_solute, jnp.float32)
        entering = jnp.concatenate([nuclei, melt], axis=0)
        moved = lax.dynamic_slice_in_dim(jnp.concatenate([field, entering], axis=3), count, NZ, axis=3)
        field = advance(moved, mobility)
    return field
```

```python
import functools

import jax
import jax.numpy as jnp
from jax import lax
from jax.experimental import pallas as pl
from jax.experimental.pallas import tpu as pltpu
from jax.sharding import PartitionSpec as P

step_rate = 0.1
stiffness = 0.7
coupling = 0.5
diffusion = 0.14
rejection = 0.5
nucleus = 0.3
melt_solute = 1.0

TILE = 8
LANES = 128
REACH = 2
GROUP = 6
SHARE = 4

VMEM = pl.BlockSpec(memory_space=pltpu.VMEM)
SMEM = pl.BlockSpec(memory_space=pltpu.SMEM)


def iota(shape, axis):
    return lax.broadcasted_iota(jnp.int32, shape, axis)


def is_even():
    return lax.rem(lax.axis_index("gx"), 2) == 0


def group_and_slot():
    lane = iota((1, LANES), 1)
    slot = lax.shift_right_logical(lane * 43, 8)
    return slot, lane - slot * GROUP


def edge_tile(ref, g, x):
    rows = ref.shape[2]
    low = ref[g, x, 0:TILE]
    high = ref[g, x, rows - TILE : rows]
    return jnp.where(iota((TILE, LANES), 0) < TILE // 2, low, high)


def corner_rows(k):
    row = iota((TILE, LANES), 0)
    return (row == 2 * k) | (row == (2 * k + TILE - 1) % TILE)


def pack_kernel(state, face_a, face_b, rows, corner_a, corner_b):
    fields, width = state.shape[:2]
    even = is_even()
    last = width - REACH
    face_a[...] = state[:, pl.ds(jnp.where(even, last, 0), REACH)]
    face_b[...] = state[:, pl.ds(jnp.where(even, 0, last), REACH)]
    row = iota((TILE, LANES), 0)
    outer = (row < REACH) | (row >= TILE - REACH)
    for g in range(fields):
        for pair in range(width // 2):
            first = edge_tile(state, g, 2 * pair)
            second = edge_tile(state, g, 2 * pair + 1)
            rows[g, pair] = jnp.where(outer, first, pltpu.roll(second, TILE // 2, 0))
    near_a = jnp.where(even, width - 1, 0)
    near_b = jnp.where(even, 0, width - 1)
    for corner, x in ((corner_a, near_a), (corner_b, near_b)):
        for t in range(corner.shape[0]):
            held = None
            for k in range(SHARE):
                g = t * SHARE + k
                if g < fields:
                    tile = edge_tile(state, g, x)
                    if k:
                        tile = jnp.where(corner_rows(k), pltpu.roll(tile, 2 * k, 0), held)
                    held = tile
            corner[t] = held


def join_kernel(merged, state, face_a, face_b, *rest):
    count = 1 if merged else 2
    rows = rest[:count]
    corner_a = rest[count : 2 * count]
    corner_b = rest[2 * count : 3 * count]
    wide, slab = rest[3 * count :]
    fields, width, height = state.shape[:3]
    even = is_even()
    upper_half = iota((TILE, LANES), 0) < TILE // 2

    def both(refs, index):
        if merged:
            return refs[0][index]
        return jnp.where(upper_half, refs[0][index], refs[1][index])

    slot_a = jnp.where(even, width + REACH, 0)
    slot_b = jnp.where(even, 0, width + REACH)
    blank = jnp.zeros((TILE, LANES), jnp.float32)
    for g in range(fields):
        wide[g, pl.ds(slot_a, REACH), 0:height] = face_a[g]
        wide[g, pl.ds(slot_b, REACH), 0:height] = face_b[g]
        for x in range(width):
            wide[g, x + REACH, 0:height] = state[g, x]
        for pair in range(width // 2):
            tile = both(rows, (g, pair))
            wide[g, 2 * pair + REACH, height : height + TILE] = tile
            wide[g, 2 * pair + 1 + REACH, height : height + TILE] = pltpu.roll(tile, TILE // 2, 0)
        wide[g, 0, height : height + TILE] = blank
        wide[g, width + 2 * REACH - 1, height : height + TILE] = blank
        t, k = g // SHARE, g % SHARE
        for refs, slot in (
            (corner_a, jnp.where(even, width + REACH, REACH - 1)),
            (corner_b, jnp.where(even, REACH - 1, width + REACH)),
        ):
            tile = both(refs, (t,))
            if k:
                tile = pltpu.roll(tile, TILE - 2 * k, 0)
            wide[g, slot, height : height + TILE] = tile
    slots, _ = group_and_slot()

    @pl.loop(0, fields)
    def _(g):
        held = jnp.zeros((height + TILE, LANES), jnp.float32)
        for slot in range(width + 2 * REACH):
            moved = pltpu.roll(wide[g, slot], (slot * GROUP + REACH) % LANES, 1)
            held = jnp.where(slots == slot, moved, held)
        slab[g] = held


def relax(phases, solute, sums, solute_sum, theta, mobility):
    squares = phases[0] * phases[0]
    for phase in phases[1:]:
        squares = squares + phase * phase
    excess = (theta - coupling * solute) - squares
    fresh = []
    fresh_squares = None
    for g, phase in enumerate(phases):
        speed = step_rate * mobility[g]
        rate = speed * excess + (1.0 - 6.0 * stiffness * speed)
        new = phase * rate + (stiffness * speed) * sums[g]()
        fresh.append(new)
        fresh_squares = new * new if fresh_squares is None else fresh_squares + new * new
    kept = (1.0 - 6.0 * diffusion) - rejection * (fresh_squares - squares)
    fresh.append(solute * kept + diffusion * solute_sum())
    return fresh


def bulk_kernel(wide, mobility, shifts, out, lower, first):
    fields, slots, rows = wide.shape[:3]
    grains = fields - 1
    width, height, length = out.shape[1:]
    span = float(length * lax.axis_size("gz"))
    base = lax.axis_index("gz") * length
    lowest = lax.axis_index("gz") == 0
    lane = iota((1, LANES), 1)
    speeds = [mobility[g] for g in range(grains)]

    def theta_of(shift):
        zpos = (base + lane - shift).astype(jnp.float32)
        return 1.0 - 2.0 * (zpos + 0.5) / span

    def bottom(active):
        return jnp.where((lane == REACH) & active, 0.0, 1.0)

    def neighbours(ref, g, x, center, mask, take):
        total = ref[g, x - 1, 0:take] + ref[g, x + 1, 0:take]
        total = total + pltpu.roll(center, 1, 0)[0:take] + pltpu.roll(center, rows - 1, 0)[0:take]
        center = center[0:take]
        return total + pltpu.roll(center, 1, 1) * mask + pltpu.roll(center, LANES - 1, 1)

    def plane(ref, x, theta, mask, take):
        full = [ref[g, x] for g in range(fields)]
        cut = [p[0:take] for p in full]
        sums = [
            functools.partial(neighbours, ref, g, x, full[g], mask, take) for g in range(fields)
        ]
        return relax(cut[:grains], cut[grains], sums[:grains], sums[grains], theta, speeds)

    theta_first = theta_of(shifts[0])
    mask_first = bottom(lowest & (shifts[0] > 0))

    @pl.loop(0, slots - 2)
    def _(x):
        fresh = plane(wide, x + 1, theta_first, mask_first, rows)
        for g in range(fields):
            first[g, x] = fresh[g]

    theta_second = theta_of(REACH)
    mask_second = bottom(lowest)

    @pl.loop(0, width)
    def _(x):
        fresh = plane(first, x + 1, theta_second, mask_second, height)
        for g in range(fields):
            out[g, x] = pltpu.roll(fresh[g], LANES - REACH, 1)

    slot_of, _ = group_and_slot()

    @pl.loop(0, fields)
    def _(g):
        held = jnp.zeros((rows, LANES), jnp.float32)
        for slot in range(1, slots - 1):
            moved = pltpu.roll(first[g, slot - 1], (slot * GROUP + REACH + 1) % LANES, 1)
            held = jnp.where(slot_of == slot, moved, held)
        lower[g] = held


def crown_kernel(done, slab, above, lower, seeds, mobility, shifts, out, crown):
    fields, rows = slab.shape[:2]
    grains = fields - 1
    width, height, length = out.shape[1:]
    total_x, total_y = seeds.shape[2:]
    span = float(length * lax.axis_size("gz"))
    base = lax.axis_index("gz") * length
    topmost = lax.axis_index("gz") == lax.axis_size("gz") - 1
    early = shifts[0] > 0
    slot, place = group_and_slot()
    speeds = [mobility[g] for g in range(grains)]

    step = jnp.where(early, 0, 1)
    row_y = iota((rows, total_y), 0)
    y = jnp.where(row_y >= height + TILE // 2, row_y - rows, row_y) + lax.axis_index("gy") * height
    y = jnp.where(y < 0, y + total_y, y)
    y = jnp.where(y >= total_y, y - total_y, y)
    pick_y = jnp.where(iota((rows, total_y), 1) == y, 1.0, 0.0)
    x = slot - REACH + lax.axis_index("gx") * width
    x = jnp.where(x < 0, x + total_x, x)
    x = jnp.where(x >= total_x, x - total_x, x)
    marks = jnp.zeros((rows, LANES), jnp.float32)
    for k in range(REACH):
        chosen = seeds[step, k].astype(jnp.float32)
        across = lax.dot_general(
            pick_y, chosen, (((1,), (1,)), ((), ())), preferred_element_type=jnp.float32
        )
        pick_x = jnp.where((iota((total_x, LANES), 0) == x) & (place == REACH + k), 1.0, 0.0)
        marks = marks + jnp.dot(across, pick_x, preferred_element_type=jnp.float32)

    def entering(g):
        if g == grains:
            return jnp.full((rows, LANES), melt_solute, jnp.float32)
        return jnp.where(marks == float(g), nucleus, 0.0)

    planted = (place >= REACH) & (place < 2 * REACH)
    zero = jnp.zeros((rows, LANES), jnp.float32)

    def theta_of(offset):
        zpos = (base + length + place - offset).astype(jnp.float32)
        return 1.0 - 2.0 * (zpos + 0.5) / span

    def around(p):
        total = pltpu.roll(p, GROUP, 1) + pltpu.roll(p, LANES - GROUP, 1)
        total = total + pltpu.roll(p, 1, 0) + pltpu.roll(p, rows - 1, 0)
        return total + pltpu.roll(p, 1, 1) + pltpu.roll(p, LANES - 1, 1)

    def advance(ps, theta):
        sums = [functools.partial(around, p) for p in ps]
        return relax(ps[:grains], ps[grains], sums[:grains], sums[grains], theta, speeds)

    before = []
    for g in range(fields):
        high = jnp.where(topmost, jnp.where(planted & early, entering(g), zero), above[g])
        before.append(jnp.where(place < REACH, slab[g], high))
    middle = advance(before, theta_of(REACH + shifts[0]))
    after = []
    for g in range(fields):
        value = middle[g]
        value = jnp.where(topmost & jnp.logical_not(early) & planted, entering(g), value)
        value = jnp.where(topmost & (place >= 2 * REACH), 0.0, value)
        after.append(jnp.where(place < REACH, lower[g], pltpu.roll(value, 1, 1)))
    final = advance(after, theta_of(REACH + 1 + REACH))
    for g in range(fields):
        crown[g] = final[g]

    top = iota((1, LANES), 1) >= LANES - 2 * REACH

    @pl.loop(0, fields)
    def _(g):
        whole = crown[g, 0:height]
        for x in range(width):
            shift = (LANES - 2 * REACH - (x + REACH) * GROUP - 1) % LANES
            out[g, x] = jnp.where(top, pltpu.roll(whole, shift, 1), done[g, x])


def shape(*dims):
    return jax.ShapeDtypeStruct(dims, jnp.float32)


def call(kernel, outs, inputs, cost, specs=None, scratch=(), aliases=None):
    return pl.pallas_call(
        kernel,
        out_shape=outs,
        in_specs=specs or [VMEM] * len(inputs),
        out_specs=jax.tree.map(lambda _: VMEM, outs),
        scratch_shapes=list(scratch),
        input_output_aliases=aliases or {},
        cost_estimate=pl.CostEstimate(flops=cost, bytes_accessed=cost, transcendentals=0),
        compiler_params=pltpu.CompilerParams(vmem_limit_bytes=24 * 1024 * 1024),
    )(*inputs)


def shards(state, mobility, seeds, frame_shifts):
    fields, width, height, length = state.shape
    count_x, count_y, count_z = (lax.axis_size(a) for a in ("gx", "gy", "gz"))
    merged = count_y == 2
    rows = height + TILE
    groups = -(-fields // SHARE)

    face_a, face_b, edge, corner_a, corner_b = call(
        pack_kernel,
        [
            shape(fields, REACH, height, length),
            shape(fields, REACH, height, length),
            shape(fields, width // 2, TILE, length),
            shape(groups, TILE, length),
            shape(groups, TILE, length),
        ],
        [state],
        100000,
    )

    def partner(i, kind):
        return (i + 1) % count_x if (i % 2 == 0) == (kind == 0) else (i - 1) % count_x

    def swap(value, kind):
        return lax.ppermute(value, "gx", [(i, partner(i, kind)) for i in range(count_x)])

    toward = [-1] if merged else [-1, 1]
    near = [
        lax.ppermute(edge, "gy", [(j, (j + d) % count_y) for j in range(count_y)]) for d in toward
    ]

    def diagonal(value, kind):
        return [
            lax.ppermute(
                value,
                ("gx", "gy"),
                [
                    (i * count_y + j, partner(i, kind) * count_y + (j + d) % count_y)
                    for i in range(count_x)
                    for j in range(count_y)
                ],
            )
            for d in toward
        ]

    got_b = swap(face_b, 1)
    got_a = swap(face_a, 0)
    far_b = diagonal(corner_b, 1)
    far_a = diagonal(corner_a, 0)

    wide, slab = call(
        functools.partial(join_kernel, merged),
        [shape(fields, width + 2 * REACH, rows, length), shape(fields, rows, length)],
        [state, got_a, got_b, *near, *far_a, *far_b],
        100000,
    )
    above = lax.ppermute(slab, "gz", [(k, k - 1) for k in range(1, count_z)])
    done, lower = call(
        bulk_kernel,
        [shape(fields, width, height, length), shape(fields, rows, length)],
        [wide, mobility, frame_shifts],
        20000000,
        specs=[VMEM, SMEM, SMEM],
        scratch=[pltpu.VMEM((fields, width + 2, rows, length), jnp.float32)],
    )
    return call(
        crown_kernel,
        shape(fields, width, height, length),
        [done, slab, above, lower, seeds, mobility, frame_shifts],
        100000,
        specs=[VMEM, VMEM, VMEM, VMEM, VMEM, SMEM, SMEM],
        scratch=[pltpu.VMEM((fields, rows, length), jnp.float32)],
        aliases={},
    )


def solution(mesh):
    placed = (P(None, "gx", "gy", "gz"), P(), P(), P())
    return jax.shard_map(
        shards, mesh=mesh, in_specs=placed, out_specs=P(None, "gx", "gy", "gz"), check_vma=False
    )
```

```python
import functools

import jax
import jax.numpy as jnp
from jax import lax
from jax.experimental import pallas as pl
from jax.experimental.pallas import tpu as pltpu
from jax.sharding import PartitionSpec as P

step_rate = 0.1
stiffness = 0.7
coupling = 0.5
diffusion = 0.14
rejection = 0.5
nucleus = 0.3
melt_solute = 1.0

TILE = 8
LANES = 128
REACH = 2
GROUP = 6
SHARE = 4

VMEM = pl.BlockSpec(memory_space=pltpu.VMEM)
SMEM = pl.BlockSpec(memory_space=pltpu.SMEM)


def iota(shape, axis):
    return lax.broadcasted_iota(jnp.int32, shape, axis)


def is_even():
    return lax.rem(lax.axis_index("gx"), 2) == 0


def group_and_slot():
    lane = iota((1, LANES), 1)
    slot = lax.shift_right_logical(lane * 43, 8)
    return slot, lane - slot * GROUP


def edge_tile(ref, g, x):
    rows = ref.shape[2]
    low = ref[g, x, 0:TILE]
    high = ref[g, x, rows - TILE : rows]
    return jnp.where(iota((TILE, LANES), 0) < TILE // 2, low, high)


def corner_rows(k):
    row = iota((TILE, LANES), 0)
    return (row == 2 * k) | (row == (2 * k + TILE - 1) % TILE)


def faces_kernel(state, face_a, face_b, sems):
    width = state.shape[1]
    even = is_even()
    last = width - REACH
    copies = [
        pltpu.make_async_copy(
            state.at[:, pl.ds(jnp.where(pick, last, 0), REACH)], face, sems.at[n]
        )
        for n, (pick, face) in enumerate(((jnp.logical_not(even), face_b), (even, face_a)))
    ]
    for copy in copies:
        copy.start()
    for copy in copies:
        copy.wait()


def rims_kernel(state, rows, corner_a, corner_b):
    fields, width = state.shape[:2]
    even = is_even()
    row = iota((TILE, LANES), 0)
    outer = (row < REACH) | (row >= TILE - REACH)
    for g in range(fields):
        for pair in range(width // 2):
            first = edge_tile(state, g, 2 * pair)
            second = edge_tile(state, g, 2 * pair + 1)
            rows[g, pair] = jnp.where(outer, first, pltpu.roll(second, TILE // 2, 0))
    near_a = jnp.where(even, width - 1, 0)
    near_b = jnp.where(even, 0, width - 1)
    for corner, x in ((corner_a, near_a), (corner_b, near_b)):
        for t in range(corner.shape[0]):
            held = None
            for k in range(SHARE):
                g = t * SHARE + k
                if g < fields:
                    tile = edge_tile(state, g, x)
                    if k:
                        tile = jnp.where(corner_rows(k), pltpu.roll(tile, 2 * k, 0), held)
                    held = tile
            corner[t] = held


def bottom_mask(active):
    return jnp.where((iota((1, LANES), 1) == REACH) & active, 0.0, 1.0)


def along(p, mask):
    return pltpu.roll(p, 1, 1) * mask + pltpu.roll(p, LANES - 1, 1)


def early_mask(shifts):
    return bottom_mask((lax.axis_index("gz") == 0) & (shifts[0] > 0))


def slot_shift(slot):
    return (slot * GROUP + REACH) % LANES


def prepare_kernel(state, seeds, shifts, zsum, own, marks):
    fields, width, height, _ = state.shape
    rows = height + TILE
    total_x, total_y = seeds.shape[2:]
    slot, place = group_and_slot()
    mask = early_mask(shifts)
    for g in range(fields):
        held = None
        for x in range(width):
            p = state[g, x]
            zsum[g, x] = along(p, mask)
            moved = pltpu.roll(p, slot_shift(x + REACH), 1)
            held = moved if held is None else jnp.where(slot == x + REACH, moved, held)
        own[g] = held

    step = jnp.where(shifts[0] > 0, 0, 1)
    row_y = iota((rows, total_y), 0)
    y = jnp.where(row_y >= height + TILE // 2, row_y - rows, row_y) + lax.axis_index("gy") * height
    y = jnp.where(y < 0, y + total_y, y)
    y = jnp.where(y >= total_y, y - total_y, y)
    pick_y = jnp.where(iota((rows, total_y), 1) == y, 1.0, 0.0)
    x = slot - REACH + lax.axis_index("gx") * width
    x = jnp.where(x < 0, x + total_x, x)
    x = jnp.where(x >= total_x, x - total_x, x)
    total = jnp.zeros((rows, LANES), jnp.float32)
    for k in range(REACH):
        chosen = seeds[step, k].astype(jnp.float32)
        across = lax.dot_general(
            pick_y, chosen, (((1,), (1,)), ((), ())), preferred_element_type=jnp.float32
        )
        pick_x = jnp.where((iota((total_x, LANES), 0) == x) & (place == REACH + k), 1.0, 0.0)
        total = total + jnp.dot(across, pick_x, preferred_element_type=jnp.float32)
    marks[...] = total


class Halo:
    def __init__(self, merged, face_a, face_b, rest):
        count = 1 if merged else 2
        self.merged = merged
        self.faces = (face_a, face_b)
        self.rows = rest[:count]
        self.corners = (rest[count : 2 * count], rest[2 * count : 3 * count])
        self.even = is_even()

    def both(self, refs, index):
        if self.merged:
            return refs[0][index]
        upper = iota((TILE, LANES), 0) < TILE // 2
        return jnp.where(upper, refs[0][index], refs[1][index])

    def face(self, g, side, n):
        a, b = (ref[g, n] for ref in self.faces)
        return jnp.where(self.even, a, b) if side else jnp.where(self.even, b, a)

    def pair(self, g, n):
        tile = self.both(self.rows, (g, n))
        return tile, pltpu.roll(tile, TILE // 2, 0)

    def corner(self, g, side):
        t, k = g // SHARE, g % SHARE
        a, b = (self.both(refs, (t,)) for refs in self.corners)
        tile = jnp.where(self.even, a, b) if side else jnp.where(self.even, b, a)
        return pltpu.roll(tile, TILE - 2 * k, 0) if k else tile


def slab_kernel(merged, own, face_a, face_b, *rest):
    slab = rest[-1]
    halo = Halo(merged, face_a, face_b, rest[:-1])
    fields, height = own.shape[:2]
    width = 2 * halo.rows[0].shape[1]
    slot, _ = group_and_slot()
    for g in range(fields):
        held = own[g]
        for side in range(2):
            for n in range(REACH):
                where = n + side * (width + REACH)
                moved = pltpu.roll(halo.face(g, side, n), slot_shift(where), 1)
                held = jnp.where(slot == where, moved, held)
        slab[g, 0:height] = held
        tiles = [(REACH - 1, halo.corner(g, 0)), (width + REACH, halo.corner(g, 1))]
        for n in range(width // 2):
            first, second = halo.pair(g, n)
            tiles += [(2 * n + REACH, first), (2 * n + 1 + REACH, second)]
        held = jnp.zeros((TILE, LANES), jnp.float32)
        for where, tile in tiles:
            held = jnp.where(slot == where, pltpu.roll(tile, slot_shift(where), 1), held)
        slab[g, height : height + TILE] = held


def relax(phases, solute, sums, solute_sum, theta, mobility):
    squares = phases[0] * phases[0]
    for phase in phases[1:]:
        squares = squares + phase * phase
    excess = (theta - coupling * solute) - squares
    fresh = []
    fresh_squares = None
    for g, phase in enumerate(phases):
        speed = step_rate * mobility[g]
        rate = speed * excess + (1.0 - 6.0 * stiffness * speed)
        new = phase * rate + (stiffness * speed) * sums[g]()
        fresh.append(new)
        fresh_squares = new * new if fresh_squares is None else fresh_squares + new * new
    kept = (1.0 - 6.0 * diffusion) - rejection * (fresh_squares - squares)
    fresh.append(solute * kept + diffusion * solute_sum())
    return fresh


def bulk_kernel(merged, state, zsum, mobility, shifts, face_a, face_b, *rest):
    done, lower, wide, first, rims, sums, pending = rest[-7:]
    halo = Halo(merged, face_a, face_b, rest[:-7])
    fields, width, height, length = state.shape
    grains = fields - 1
    rows = height + TILE
    top = height + TILE
    span = float(length * lax.axis_size("gz"))
    base = lax.axis_index("gz") * length
    lane = iota((1, LANES), 1)
    slot_of, _ = group_and_slot()
    speeds = [mobility[g] for g in range(grains)]
    own = slice(TILE, TILE + height)

    def theta_of(shift):
        zpos = (base + lane - shift).astype(jnp.float32)
        return 1.0 - 2.0 * (zpos + 0.5) / span

    def put_rim(ref, g, x, tile):
        ref[g, x, 0:TILE] = tile
        ref[g, x, top : top + TILE] = tile

    for g in range(fields):
        for x in range(width):
            wide[g, x + REACH, own] = state[g, x]
        for side in range(2):
            for n in range(REACH):
                wide[g, n + side * (width + REACH), own] = halo.face(g, side, n)
        for n in range(width // 2):
            first_tile, second_tile = halo.pair(g, n)
            put_rim(wide, g, 2 * n + REACH, first_tile)
            put_rim(wide, g, 2 * n + 1 + REACH, second_tile)
        put_rim(wide, g, REACH - 1, halo.corner(g, 0))
        put_rim(wide, g, width + REACH, halo.corner(g, 1))
        for x in (0, width + 2 * REACH - 1):
            put_rim(wide, g, x, jnp.zeros((TILE, LANES), jnp.float32))

    mask_first = early_mask(shifts)
    theta_first = theta_of(shifts[0])

    def lateral(ref, g, x, with_rim):
        total = ref[g, x - 1, own] + ref[g, x + 1, own]
        total = total + ref[g, x, TILE - 1 : top - 1] + ref[g, x, TILE + 1 : top + 1]
        if not with_rim:
            return total
        rim = ref[g, x - 1, 0:TILE] + ref[g, x + 1, 0:TILE]
        rim = rim + ref[g, x, top - 1 : top - 1 + TILE] + ref[g, x, 1 : TILE + 1]
        return jnp.concatenate([total, rim], axis=0)

    def plane_first(x, zsum_own, zsum_rim):
        full = [wide[g, x, TILE : top + TILE] for g in range(fields)]
        parts = [
            lambda g=g: lateral(wide, g, x, True)
            + jnp.concatenate([zsum_own(g), zsum_rim(g)], axis=0)
            for g in range(fields)
        ]
        fresh = relax(full[:grains], full[grains], parts[:grains], parts[grains], theta_first, speeds)
        for g in range(fields):
            first[g, x - 1, own] = fresh[g][0:height]
            put_rim(first, g, x - 1, fresh[g][height:rows])

    def put_lower(slot, source):
        for g in range(fields):
            moved = pltpu.roll(source(g), slot, 1)
            lower[g] = jnp.where(slot_of * GROUP + REACH + 1 == slot, moved, lower[g])

    lower[...] = jnp.zeros_like(lower)
    for x in (1, width + REACH):
        plane_first(
            x,
            lambda g, x=x: along(wide[g, x, own], mask_first),
            lambda g, x=x: along(wide[g, x, 0:TILE], mask_first),
        )
    for g in range(fields):
        rims[0, g] = along(wide[g, REACH, 0:TILE], mask_first)
        sums[0, g] = jnp.zeros((height, LANES), jnp.float32)

    def plane_of(x):
        return lambda g: jnp.concatenate([first[g, x, own], first[g, x, 0:TILE]], axis=0)

    @pl.loop(0, width)
    def _(x):
        now = lax.rem(x, 2)
        put_lower((x + 1) * GROUP + REACH + 1, plane_of(x))
        plane_first(x + REACH, lambda g: zsum[g, x], lambda g: rims[now, g])
        for g in range(fields):
            rims[1 - now, g] = along(wide[g, x + REACH + 1, 0:TILE], mask_first)

    for x in (width, width + 1):
        put_lower((x + 1) * GROUP + REACH + 1, plane_of(x))

    theta_second = theta_of(REACH)
    mask_second = bottom_mask(lax.axis_index("gz") == 0)

    for g in range(fields):
        sums[0, g] = along(first[g, 1, own], mask_second)
        pending[0, g] = jnp.zeros((height, LANES), jnp.float32)

    def flush(now, x):
        for g in range(fields):
            done[g, x] = pltpu.roll(pending[now, g], LANES - REACH, 1)

    @pl.loop(0, width)
    def _(x):
        now = lax.rem(x, 2)
        flush(now, jnp.maximum(x - 1, 0))
        full = [first[g, x + 1, own] for g in range(fields)]
        parts = [
            lambda g=g: lateral(first, g, x + 1, False) + sums[now, g] for g in range(fields)
        ]
        fresh = relax(full[:grains], full[grains], parts[:grains], parts[grains], theta_second, speeds)
        for g in range(fields):
            pending[1 - now, g] = fresh[g]
            sums[1 - now, g] = along(first[g, x + 2, own], mask_second)

    flush(width % 2, width - 1)


def crown_kernel(done, slab, above, lower, marks, mobility, shifts, out, whole, sems):
    fields, rows = slab.shape[:2]
    grains = fields - 1
    width, height, length = done.shape[1:]
    span = float(length * lax.axis_size("gz"))
    base = lax.axis_index("gz") * length
    topmost = lax.axis_index("gz") == lax.axis_size("gz") - 1
    early = shifts[0] > 0
    _, place = group_and_slot()
    speeds = [mobility[g] for g in range(grains)]

    def entering(g):
        if g == grains:
            return jnp.full((rows, LANES), melt_solute, jnp.float32)
        return jnp.where(marks[...] == float(g), nucleus, 0.0)

    planted = (place >= REACH) & (place < 2 * REACH)
    zero = jnp.zeros((rows, LANES), jnp.float32)

    def theta_of(offset):
        zpos = (base + length + place - offset).astype(jnp.float32)
        return 1.0 - 2.0 * (zpos + 0.5) / span

    def around(p):
        total = pltpu.roll(p, GROUP, 1) + pltpu.roll(p, LANES - GROUP, 1)
        total = total + pltpu.roll(p, 1, 0) + pltpu.roll(p, rows - 1, 0)
        return total + pltpu.roll(p, 1, 1) + pltpu.roll(p, LANES - 1, 1)

    def advance(ps, theta):
        sums = [functools.partial(around, p) for p in ps]
        return relax(ps[:grains], ps[grains], sums[:grains], sums[grains], theta, speeds)

    before = []
    for g in range(fields):
        high = jnp.where(topmost, jnp.where(planted & early, entering(g), zero), above[g])
        before.append(jnp.where(place < REACH, slab[g], high))
    middle = advance(before, theta_of(REACH + shifts[0]))
    after = []
    for g in range(fields):
        value = middle[g]
        value = jnp.where(topmost & jnp.logical_not(early) & planted, entering(g), value)
        value = jnp.where(topmost & (place >= 2 * REACH), 0.0, value)
        after.append(jnp.where(place < REACH, lower[g], pltpu.roll(value, 1, 1)))
    final = advance(after, theta_of(REACH + 1 + REACH))

    top = iota((1, LANES), 1) >= LANES - 2 * REACH
    copies = []
    for g in range(fields):
        cut = final[g][0:height]
        for x in range(width):
            shift = (LANES - 2 * REACH - (x + REACH) * GROUP - 1) % LANES
            whole[g, x] = jnp.where(top, pltpu.roll(cut, shift, 1), done[g, x])
        copy = pltpu.make_async_copy(whole.at[g], out.at[g], sems.at[g])
        copy.start()
        copies.append(copy)
    for copy in copies:
        copy.wait()


def shape(*dims):
    return jax.ShapeDtypeStruct(dims, jnp.float32)


def call(kernel, outs, inputs, cost, specs=None, outs_specs=None, scratch=()):
    return pl.pallas_call(
        kernel,
        out_shape=outs,
        in_specs=specs or [VMEM] * len(inputs),
        out_specs=outs_specs or jax.tree.map(lambda _: VMEM, outs),
        scratch_shapes=list(scratch),
        cost_estimate=pl.CostEstimate(flops=cost, bytes_accessed=cost, transcendentals=0),
        compiler_params=pltpu.CompilerParams(vmem_limit_bytes=24 * 1024 * 1024),
    )(*inputs)


def shards(state, mobility, seeds, frame_shifts):
    fields, width, height, length = state.shape
    count_x, count_y, count_z = (lax.axis_size(a) for a in ("gx", "gy", "gz"))
    merged = count_y == 2
    rows = height + TILE
    groups = -(-fields // SHARE)
    block = shape(fields, width, height, length)
    packed = shape(fields, rows, length)

    def partner(i, kind):
        return (i + 1) % count_x if (i % 2 == 0) == (kind == 0) else (i - 1) % count_x

    def swap(value, kind):
        return lax.ppermute(value, "gx", [(i, partner(i, kind)) for i in range(count_x)])

    toward = [-1] if merged else [-1, 1]

    def diagonal(value, kind):
        return [
            lax.ppermute(
                value,
                ("gx", "gy"),
                [
                    (i * count_y + j, partner(i, kind) * count_y + (j + d) % count_y)
                    for i in range(count_x)
                    for j in range(count_y)
                ],
            )
            for d in toward
        ]

    face_a, face_b = call(
        faces_kernel,
        [shape(fields, REACH, height, length)] * 2,
        [state],
        100000,
        specs=[pl.BlockSpec(memory_space=pltpu.HBM)],
        scratch=[pltpu.SemaphoreType.DMA((2,))],
    )
    got_b = swap(face_b, 1)
    edge, corner_a, corner_b = call(
        rims_kernel,
        [
            shape(fields, width // 2, TILE, length),
            shape(groups, TILE, length),
            shape(groups, TILE, length),
        ],
        [state],
        100000,
    )
    near = [
        lax.ppermute(edge, "gy", [(j, (j + d) % count_y) for j in range(count_y)]) for d in toward
    ]
    got_a = swap(face_a, 0)
    far_b = diagonal(corner_b, 1)
    far_a = diagonal(corner_a, 0)
    zsum, own, marks = call(
        prepare_kernel,
        [block, shape(fields, height, length), shape(rows, length)],
        [state, seeds, frame_shifts],
        5000000,
        specs=[VMEM, VMEM, SMEM],
    )
    halo = [got_a, got_b, *near, *far_a, *far_b]
    slab = call(functools.partial(slab_kernel, merged), packed, [own, *halo], 100000)
    above = lax.ppermute(slab, "gz", [(k, k - 1) for k in range(1, count_z)])
    done, lower = call(
        functools.partial(bulk_kernel, merged),
        [block, packed],
        [state, zsum, mobility, frame_shifts, *halo],
        20000000,
        specs=[VMEM, VMEM, SMEM, SMEM] + [VMEM] * len(halo),
        scratch=[
            pltpu.VMEM((fields, width + 2 * REACH, rows + TILE, length), jnp.float32),
            pltpu.VMEM((fields, width + 2, rows + TILE, length), jnp.float32),
            pltpu.VMEM((2, fields, TILE, length), jnp.float32),
            pltpu.VMEM((2, fields, height, length), jnp.float32),
            pltpu.VMEM((2, fields, height, length), jnp.float32),
        ],
    )
    return call(
        crown_kernel,
        block,
        [done, slab, above, lower, marks, mobility, frame_shifts],
        100000,
        specs=[VMEM] * 5 + [SMEM, SMEM],
        outs_specs=pl.BlockSpec(memory_space=pltpu.HBM),
        scratch=[
            pltpu.VMEM((fields, width, height, length), jnp.float32),
            pltpu.SemaphoreType.DMA((fields,)),
        ],
    )


def solution(mesh):
    placed = (P(None, "gx", "gy", "gz"), P(), P(), P())
    return jax.shard_map(
        shards, mesh=mesh, in_specs=placed, out_specs=P(None, "gx", "gy", "gz"), check_vma=False
    )
```

```python
import functools

import jax
import jax.numpy as jnp
from jax import lax
from jax.experimental import pallas as pl
from jax.experimental.pallas import tpu as pltpu
from jax.sharding import PartitionSpec as P


step_rate = 0.1
stiffness = 0.7
coupling = 0.5
diffusion = 0.14
rejection = 0.5
nucleus = 0.3
melt_solute = 1.0

TILE = 8
LANES = 128
REACH = 2
GROUP = 6
SHARE = 4
UNROLL = 8

VMEM = pl.BlockSpec(memory_space=pltpu.VMEM)
SMEM = pl.BlockSpec(memory_space=pltpu.SMEM)


def iota(shape, axis):
    return lax.broadcasted_iota(jnp.int32, shape, axis)


def is_even():
    return lax.rem(lax.axis_index("gx"), 2) == 0


def group_and_slot():
    lane = iota((1, LANES), 1)
    slot = lax.shift_right_logical(lane * 43, 8)
    return slot, lane - slot * GROUP


def edge_tile(ref, g, x):
    rows = ref.shape[2]
    low = ref[g, x, 0:TILE]
    high = ref[g, x, rows - TILE : rows]
    return jnp.where(iota((TILE, LANES), 0) < TILE // 2, low, high)


def corner_rows(k):
    row = iota((TILE, LANES), 0)
    return (row == 2 * k) | (row == (2 * k + TILE - 1) % TILE)


def faces_kernel(state, face_a, face_b, sems):
    width = state.shape[1]
    even = is_even()
    last = width - REACH
    copies = [
        pltpu.make_async_copy(
            state.at[:, pl.ds(jnp.where(pick, last, 0), REACH)], face, sems.at[n]
        )
        for n, (pick, face) in enumerate(((jnp.logical_not(even), face_b), (even, face_a)))
    ]
    for copy in copies:
        copy.start()
    for copy in copies:
        copy.wait()


def rims_kernel(state, rows, corner_a, corner_b):
    fields, width = state.shape[:2]
    even = is_even()
    row = iota((TILE, LANES), 0)
    outer = (row < REACH) | (row >= TILE - REACH)
    for g in range(fields):
        for pair in range(width // 2):
            first = edge_tile(state, g, 2 * pair)
            second = edge_tile(state, g, 2 * pair + 1)
            rows[g, pair] = jnp.where(outer, first, pltpu.roll(second, TILE // 2, 0))
    near_a = jnp.where(even, width - 1, 0)
    near_b = jnp.where(even, 0, width - 1)
    for corner, x in ((corner_a, near_a), (corner_b, near_b)):
        for t in range(corner.shape[0]):
            held = None
            for k in range(SHARE):
                g = t * SHARE + k
                if g < fields:
                    tile = edge_tile(state, g, x)
                    if k:
                        tile = jnp.where(corner_rows(k), pltpu.roll(tile, 2 * k, 0), held)
                    held = tile
            corner[t] = held


def bottom_mask(active):
    return jnp.where((iota((1, LANES), 1) == REACH) & active, 0.0, 1.0)


def along(p, mask):
    return pltpu.roll(p, 1, 1) * mask + pltpu.roll(p, LANES - 1, 1)


def early_mask(shifts):
    return bottom_mask((lax.axis_index("gz") == 0) & (shifts[0] > 0))


def slot_shift(slot):
    return (slot * GROUP + REACH) % LANES


def prepare_kernel(state, seeds, shifts, zsum, own, marks):
    fields, width, height, _ = state.shape
    rows = height + TILE
    total_x, total_y = seeds.shape[2:]
    slot, place = group_and_slot()
    mask = early_mask(shifts)
    for g in range(fields):
        held = None
        for x in range(width):
            p = state[g, x]
            zsum[g, x] = along(p, mask)
            moved = pltpu.roll(p, slot_shift(x + REACH), 1)
            held = moved if held is None else jnp.where(slot == x + REACH, moved, held)
        own[g] = held

    step = jnp.where(shifts[0] > 0, 0, 1)
    row_y = iota((rows, total_y), 0)
    y = jnp.where(row_y >= height + TILE // 2, row_y - rows, row_y) + lax.axis_index("gy") * height
    y = jnp.where(y < 0, y + total_y, y)
    y = jnp.where(y >= total_y, y - total_y, y)
    pick_y = jnp.where(iota((rows, total_y), 1) == y, 1.0, 0.0)
    x = slot - REACH + lax.axis_index("gx") * width
    x = jnp.where(x < 0, x + total_x, x)
    x = jnp.where(x >= total_x, x - total_x, x)
    total = jnp.zeros((rows, LANES), jnp.float32)
    for k in range(REACH):
        chosen = seeds[step, k].astype(jnp.float32)
        across = lax.dot_general(
            pick_y, chosen, (((1,), (1,)), ((), ())), preferred_element_type=jnp.float32
        )
        pick_x = jnp.where((iota((total_x, LANES), 0) == x) & (place == REACH + k), 1.0, 0.0)
        total = total + jnp.dot(across, pick_x, preferred_element_type=jnp.float32)
    marks[...] = total


class Halo:
    def __init__(self, merged, face_a, face_b, rest):
        count = 1 if merged else 2
        self.merged = merged
        self.faces = (face_a, face_b)
        self.rows = rest[:count]
        self.corners = (rest[count : 2 * count], rest[2 * count : 3 * count])
        self.even = is_even()

    def both(self, refs, index):
        if self.merged:
            return refs[0][index]
        upper = iota((TILE, LANES), 0) < TILE // 2
        return jnp.where(upper, refs[0][index], refs[1][index])

    def face(self, g, side, n):
        a, b = (ref[g, n] for ref in self.faces)
        return jnp.where(self.even, a, b) if side else jnp.where(self.even, b, a)

    def pair(self, g, n):
        tile = self.both(self.rows, (g, n))
        return tile, pltpu.roll(tile, TILE // 2, 0)

    def corner(self, g, side):
        t, k = g // SHARE, g % SHARE
        a, b = (self.both(refs, (t,)) for refs in self.corners)
        tile = jnp.where(self.even, a, b) if side else jnp.where(self.even, b, a)
        return pltpu.roll(tile, TILE - 2 * k, 0) if k else tile


def slab_kernel(merged, own, face_a, face_b, *rest):
    slab = rest[-1]
    halo = Halo(merged, face_a, face_b, rest[:-1])
    fields, height = own.shape[:2]
    width = 2 * halo.rows[0].shape[1]
    slot, _ = group_and_slot()
    for g in range(fields):
        held = own[g]
        for side in range(2):
            for n in range(REACH):
                where = n + side * (width + REACH)
                moved = pltpu.roll(halo.face(g, side, n), slot_shift(where), 1)
                held = jnp.where(slot == where, moved, held)
        slab[g, 0:height] = held
        tiles = [(REACH - 1, halo.corner(g, 0)), (width + REACH, halo.corner(g, 1))]
        for n in range(width // 2):
            first, second = halo.pair(g, n)
            tiles += [(2 * n + REACH, first), (2 * n + 1 + REACH, second)]
        held = jnp.zeros((TILE, LANES), jnp.float32)
        for where, tile in tiles:
            held = jnp.where(slot == where, pltpu.roll(tile, slot_shift(where), 1), held)
        slab[g, height : height + TILE] = held


def relax(phases, solute, sums, solute_sum, theta, mobility):
    squares = phases[0] * phases[0]
    for phase in phases[1:]:
        squares = squares + phase * phase
    excess = (theta - coupling * solute) - squares
    fresh = []
    fresh_squares = None
    for g, phase in enumerate(phases):
        speed = step_rate * mobility[g]
        rate = speed * excess + (1.0 - 6.0 * stiffness * speed)
        new = phase * rate + (stiffness * speed) * sums[g]()
        fresh.append(new)
        fresh_squares = new * new if fresh_squares is None else fresh_squares + new * new
    kept = (1.0 - 6.0 * diffusion) - rejection * (fresh_squares - squares)
    fresh.append(solute * kept + diffusion * solute_sum())
    return fresh


def bulk_kernel(merged, state, zsum, mobility, shifts, face_a, face_b, *rest):
    done, lower, wide, first = rest[-10:-6]
    rims, sums, pending = rest[-6:-4], rest[-4:-2], rest[-2:]
    halo = Halo(merged, face_a, face_b, rest[:-10])
    fields, width, height, length = state.shape
    grains = fields - 1
    rows = height + TILE
    top = height + TILE
    span = float(length * lax.axis_size("gz"))
    base = lax.axis_index("gz") * length
    lane = iota((1, LANES), 1)
    slot_of, _ = group_and_slot()
    speeds = [mobility[g] for g in range(grains)]
    own = slice(TILE, TILE + height)

    def theta_of(shift):
        zpos = (base + lane - shift).astype(jnp.float32)
        return 1.0 - 2.0 * (zpos + 0.5) / span

    def put_rim(ref, g, x, tile):
        ref[g, x, 0:TILE] = tile
        ref[g, x, top : top + TILE] = tile

    for g in range(fields):
        for x in range(width):
            wide[g, x + REACH, own] = state[g, x]
        for side in range(2):
            for n in range(REACH):
                wide[g, n + side * (width + REACH), own] = halo.face(g, side, n)
        for n in range(width // 2):
            first_tile, second_tile = halo.pair(g, n)
            put_rim(wide, g, 2 * n + REACH, first_tile)
            put_rim(wide, g, 2 * n + 1 + REACH, second_tile)
        put_rim(wide, g, REACH - 1, halo.corner(g, 0))
        put_rim(wide, g, width + REACH, halo.corner(g, 1))
        for x in (0, width + 2 * REACH - 1):
            put_rim(wide, g, x, jnp.zeros((TILE, LANES), jnp.float32))

    mask_first = early_mask(shifts)
    theta_first = theta_of(shifts[0])

    def lateral(ref, g, x, with_rim):
        total = ref[g, x - 1, own] + ref[g, x + 1, own]
        total = total + ref[g, x, TILE - 1 : top - 1] + ref[g, x, TILE + 1 : top + 1]
        if not with_rim:
            return total
        rim = ref[g, x - 1, 0:TILE] + ref[g, x + 1, 0:TILE]
        rim = rim + ref[g, x, top - 1 : top - 1 + TILE] + ref[g, x, 1 : TILE + 1]
        return jnp.concatenate([total, rim], axis=0)

    def plane_first(x, zsum_own, zsum_rim):
        full = [wide[g, x, TILE : top + TILE] for g in range(fields)]
        parts = [
            lambda g=g: lateral(wide, g, x, True)
            + jnp.concatenate([zsum_own(g), zsum_rim(g)], axis=0)
            for g in range(fields)
        ]
        fresh = relax(full[:grains], full[grains], parts[:grains], parts[grains], theta_first, speeds)
        for g in range(fields):
            first[g, x - 1, own] = fresh[g][0:height]
            put_rim(first, g, x - 1, fresh[g][height:rows])

    def put_lower(slot, source):
        for g in range(fields):
            moved = pltpu.roll(source(g), slot, 1)
            lower[g] = jnp.where(slot_of * GROUP + REACH + 1 == slot, moved, lower[g])

    lower[...] = jnp.zeros_like(lower)
    for x in (1, width + REACH):
        plane_first(
            x,
            lambda g, x=x: along(wide[g, x, own], mask_first),
            lambda g, x=x: along(wide[g, x, 0:TILE], mask_first),
        )
    for g in range(fields):
        rims[0][g] = along(wide[g, REACH, 0:TILE], mask_first)

    def plane_of(x):
        return lambda g: jnp.concatenate([first[g, x, own], first[g, x, 0:TILE]], axis=0)

    @pl.loop(0, width // UNROLL)
    def _(block):
        for part in range(UNROLL):
            x = block * UNROLL + part
            now, after = rims[part % 2], rims[1 - part % 2]
            put_lower((x + 1) * GROUP + REACH + 1, plane_of(x))
            plane_first(x + REACH, lambda g: zsum[g, x], lambda g: now[g])
            for g in range(fields):
                after[g] = along(wide[g, x + REACH + 1, 0:TILE], mask_first)

    for x in (width, width + 1):
        put_lower((x + 1) * GROUP + REACH + 1, plane_of(x))

    theta_second = theta_of(REACH)
    mask_second = bottom_mask(lax.axis_index("gz") == 0)

    for g in range(fields):
        sums[0][g] = along(first[g, 1, own], mask_second)
        pending[1][g] = jnp.zeros((height, LANES), jnp.float32)

    def flush(held, x):
        for g in range(fields):
            done[g, x] = pltpu.roll(held[g], LANES - REACH, 1)

    @pl.loop(0, width // UNROLL)
    def _(block):
        for part in range(UNROLL):
            x = block * UNROLL + part
            now, after = part % 2, 1 - part % 2
            flush(pending[after], jnp.maximum(x - 1, 0))
            full = [first[g, x + 1, own] for g in range(fields)]
            parts = [
                lambda g=g: lateral(first, g, x + 1, False) + sums[now][g] for g in range(fields)
            ]
            fresh = relax(
                full[:grains], full[grains], parts[:grains], parts[grains], theta_second, speeds
            )
            for g in range(fields):
                pending[now][g] = fresh[g]
                sums[after][g] = along(first[g, x + 2, own], mask_second)

    flush(pending[1], width - 1)


def crown_kernel(done, slab, above, lower, marks, mobility, shifts, out, whole, sems):
    fields, rows = slab.shape[:2]
    grains = fields - 1
    width, height, length = done.shape[1:]
    span = float(length * lax.axis_size("gz"))
    base = lax.axis_index("gz") * length
    topmost = lax.axis_index("gz") == lax.axis_size("gz") - 1
    early = shifts[0] > 0
    _, place = group_and_slot()
    speeds = [mobility[g] for g in range(grains)]

    def entering(g):
        if g == grains:
            return jnp.full((rows, LANES), melt_solute, jnp.float32)
        return jnp.where(marks[...] == float(g), nucleus, 0.0)

    planted = (place >= REACH) & (place < 2 * REACH)
    zero = jnp.zeros((rows, LANES), jnp.float32)

    def theta_of(offset):
        zpos = (base + length + place - offset).astype(jnp.float32)
        return 1.0 - 2.0 * (zpos + 0.5) / span

    def around(p):
        total = pltpu.roll(p, GROUP, 1) + pltpu.roll(p, LANES - GROUP, 1)
        total = total + pltpu.roll(p, 1, 0) + pltpu.roll(p, rows - 1, 0)
        return total + pltpu.roll(p, 1, 1) + pltpu.roll(p, LANES - 1, 1)

    def advance(ps, theta):
        sums = [functools.partial(around, p) for p in ps]
        return relax(ps[:grains], ps[grains], sums[:grains], sums[grains], theta, speeds)

    before = []
    for g in range(fields):
        high = jnp.where(topmost, jnp.where(planted & early, entering(g), zero), above[g])
        before.append(jnp.where(place < REACH, slab[g], high))
    middle = advance(before, theta_of(REACH + shifts[0]))
    after = []
    for g in range(fields):
        value = middle[g]
        value = jnp.where(topmost & jnp.logical_not(early) & planted, entering(g), value)
        value = jnp.where(topmost & (place >= 2 * REACH), 0.0, value)
        after.append(jnp.where(place < REACH, lower[g], pltpu.roll(value, 1, 1)))
    final = advance(after, theta_of(REACH + 1 + REACH))

    top = iota((1, LANES), 1) >= LANES - 2 * REACH
    copies = []
    for g in range(fields):
        cut = final[g][0:height]
        for x in range(width):
            shift = (LANES - 2 * REACH - (x + REACH) * GROUP - 1) % LANES
            whole[g, x] = jnp.where(top, pltpu.roll(cut, shift, 1), done[g, x])
        copy = pltpu.make_async_copy(whole.at[g], out.at[g], sems.at[g])
        copy.start()
        copies.append(copy)
    for copy in copies:
        copy.wait()


def shape(*dims):
    return jax.ShapeDtypeStruct(dims, jnp.float32)


def call(kernel, outs, inputs, cost, specs=None, outs_specs=None, scratch=(), grant=24 << 20):
    return pl.pallas_call(
        kernel,
        out_shape=outs,
        in_specs=specs or [VMEM] * len(inputs),
        out_specs=outs_specs or jax.tree.map(lambda _: VMEM, outs),
        scratch_shapes=list(scratch),
        cost_estimate=pl.CostEstimate(flops=cost, bytes_accessed=cost, transcendentals=0),
        compiler_params=pltpu.CompilerParams(vmem_limit_bytes=grant),
    )(*inputs)


def shards(state, mobility, seeds, frame_shifts):
    fields, width, height, length = state.shape
    count_x, count_y, count_z = (lax.axis_size(a) for a in ("gx", "gy", "gz"))
    merged = count_y == 2
    rows = height + TILE
    groups = -(-fields // SHARE)
    block = shape(fields, width, height, length)
    packed = shape(fields, rows, length)

    def partner(i, kind):
        return (i + 1) % count_x if (i % 2 == 0) == (kind == 0) else (i - 1) % count_x

    def swap(value, kind):
        return lax.ppermute(value, "gx", [(i, partner(i, kind)) for i in range(count_x)])

    toward = [-1] if merged else [-1, 1]

    def diagonal(value, kind):
        return [
            lax.ppermute(
                value,
                ("gx", "gy"),
                [
                    (i * count_y + j, partner(i, kind) * count_y + (j + d) % count_y)
                    for i in range(count_x)
                    for j in range(count_y)
                ],
            )
            for d in toward
        ]

    face_a, face_b = call(
        faces_kernel,
        [shape(fields, REACH, height, length)] * 2,
        [state],
        100000,
        specs=[pl.BlockSpec(memory_space=pltpu.HBM)],
        scratch=[pltpu.SemaphoreType.DMA((2,))],
    )
    got_b = swap(face_b, 1)
    edge, corner_a, corner_b = call(
        rims_kernel,
        [
            shape(fields, width // 2, TILE, length),
            shape(groups, TILE, length),
            shape(groups, TILE, length),
        ],
        [state],
        100000,
    )
    near = [
        lax.ppermute(edge, "gy", [(j, (j + d) % count_y) for j in range(count_y)])
        for d in toward
    ]
    got_a = swap(face_a, 0)
    far_b = diagonal(corner_b, 1)
    far_a = diagonal(corner_a, 0)
    zsum, own, marks = call(
        prepare_kernel,
        [block, shape(fields, height, length), shape(rows, length)],
        [state, seeds, frame_shifts],
        5000000,
        specs=[VMEM, VMEM, SMEM],
    )
    halo = [got_a, got_b, *near, *far_a, *far_b]
    slab = call(functools.partial(slab_kernel, merged), packed, [own, *halo], 100000)
    above = lax.ppermute(slab, "gz", [(k, k - 1) for k in range(1, count_z)])
    done, lower = call(
        functools.partial(bulk_kernel, merged),
        [block, packed],
        [state, zsum, mobility, frame_shifts, *halo],
        20000000,
        specs=[VMEM, VMEM, SMEM, SMEM] + [VMEM] * len(halo),
        scratch=[
            pltpu.VMEM((fields, width + 2 * REACH, rows + TILE, length), jnp.float32),
            pltpu.VMEM((fields, width + 2, rows + TILE, length), jnp.float32),
        ]
        + [pltpu.VMEM((fields, TILE, length), jnp.float32)] * 2
        + [pltpu.VMEM((fields, height, length), jnp.float32)] * 4,
    )
    return call(
        crown_kernel,
        block,
        [done, slab, above, lower, marks, mobility, frame_shifts],
        100000,
        specs=[VMEM] * 5 + [SMEM, SMEM],
        outs_specs=pl.BlockSpec(memory_space=pltpu.HBM),
        scratch=[
            pltpu.VMEM((fields, width, height, length), jnp.float32),
            pltpu.SemaphoreType.DMA((fields,)),
        ],
    )


def solution(mesh):
    placed = (P(None, "gx", "gy", "gz"), P(), P(), P())
    return jax.shard_map(
        shards, mesh=mesh, in_specs=placed, out_specs=P(None, "gx", "gy", "gz"), check_vma=False
    )
```

```python
import functools

import jax
import jax.numpy as jnp
from jax import lax
from jax.experimental import pallas as pl
from jax.experimental.pallas import tpu as pltpu
from jax.sharding import PartitionSpec as P


step_rate = 0.1
stiffness = 0.7
coupling = 0.5
diffusion = 0.14
rejection = 0.5
nucleus = 0.3
melt_solute = 1.0

TILE = 8
LANES = 128
REACH = 2
GROUP = 6
SHARE = 4
UNROLL = 8

VMEM = pl.BlockSpec(memory_space=pltpu.VMEM)
SMEM = pl.BlockSpec(memory_space=pltpu.SMEM)


def iota(shape, axis):
    return lax.broadcasted_iota(jnp.int32, shape, axis)


def is_even():
    return lax.rem(lax.axis_index("gx"), 2) == 0


def group_and_slot():
    lane = iota((1, LANES), 1)
    slot = lax.shift_right_logical(lane * 43, 8)
    return slot, lane - slot * GROUP


def edge_tile(ref, g, x):
    rows = ref.shape[2]
    low = ref[g, x, 0:TILE]
    high = ref[g, x, rows - TILE : rows]
    return jnp.where(iota((TILE, LANES), 0) < TILE // 2, low, high)


def corner_rows(k):
    row = iota((TILE, LANES), 0)
    return (row == 2 * k) | (row == (2 * k + TILE - 1) % TILE)


def load_kernel(state, block, face_a, face_b, rows, corner_a, corner_b, sems):
    fields, width = state.shape[:2]
    even = is_even()
    last = width - REACH
    copies = [
        pltpu.make_async_copy(state.at[g], block.at[g], sems.at[g]) for g in range(fields)
    ]
    for copy in copies:
        copy.start()
    row = iota((TILE, LANES), 0)
    outer = (row < REACH) | (row >= TILE - REACH)
    near_a = jnp.where(even, width - 1, 0)
    near_b = jnp.where(even, 0, width - 1)
    held = [None, None]
    for g in range(fields):
        copies[g].wait()
        face_a[g] = block[g, pl.ds(jnp.where(even, last, 0), REACH)]
        face_b[g] = block[g, pl.ds(jnp.where(even, 0, last), REACH)]
        for pair in range(width // 2):
            first = edge_tile(block, g, 2 * pair)
            second = edge_tile(block, g, 2 * pair + 1)
            rows[g, pair] = jnp.where(outer, first, pltpu.roll(second, TILE // 2, 0))
        t, k = g // SHARE, g % SHARE
        for n, (corner, x) in enumerate(((corner_a, near_a), (corner_b, near_b))):
            tile = edge_tile(block, g, x)
            if k:
                tile = jnp.where(corner_rows(k), pltpu.roll(tile, 2 * k, 0), held[n])
            held[n] = tile
            if k == SHARE - 1 or g == fields - 1:
                corner[t] = tile


def bottom_mask(active):
    return jnp.where((iota((1, LANES), 1) == REACH) & active, 0.0, 1.0)


def along(p, mask):
    return pltpu.roll(p, 1, 1) * mask + pltpu.roll(p, LANES - 1, 1)


def early_mask(shifts):
    return bottom_mask((lax.axis_index("gz") == 0) & (shifts[0] > 0))


def slot_shift(slot):
    return (slot * GROUP + REACH) % LANES


def prepare_kernel(state, seeds, shifts, zsum, own, marks):
    fields, width, height, _ = state.shape
    rows = height + TILE
    total_x, total_y = seeds.shape[2:]
    slot, place = group_and_slot()
    mask = early_mask(shifts)
    for g in range(fields):
        held = None
        for x in range(width):
            p = state[g, x]
            zsum[g, x] = along(p, mask)
            moved = pltpu.roll(p, slot_shift(x + REACH), 1)
            held = moved if held is None else jnp.where(slot == x + REACH, moved, held)
        own[g] = held

    step = jnp.where(shifts[0] > 0, 0, 1)
    row_y = iota((rows, total_y), 0)
    y = jnp.where(row_y >= height + TILE // 2, row_y - rows, row_y) + lax.axis_index("gy") * height
    y = jnp.where(y < 0, y + total_y, y)
    y = jnp.where(y >= total_y, y - total_y, y)
    pick_y = jnp.where(iota((rows, total_y), 1) == y, 1.0, 0.0)
    x = slot - REACH + lax.axis_index("gx") * width
    x = jnp.where(x < 0, x + total_x, x)
    x = jnp.where(x >= total_x, x - total_x, x)
    total = jnp.zeros((rows, LANES), jnp.float32)
    for k in range(REACH):
        chosen = seeds[step, k].astype(jnp.float32)
        across = lax.dot_general(
            pick_y, chosen, (((1,), (1,)), ((), ())), preferred_element_type=jnp.float32
        )
        pick_x = jnp.where((iota((total_x, LANES), 0) == x) & (place == REACH + k), 1.0, 0.0)
        total = total + jnp.dot(across, pick_x, preferred_element_type=jnp.float32)
    marks[...] = total


class Halo:
    def __init__(self, merged, face_a, face_b, face_w, rest):
        count = 1 if merged else 2
        self.merged = merged
        self.faces = (face_a, face_b, face_w)
        i = lax.axis_index("gx")
        self.closing = (i == 0) | (i == lax.axis_size("gx") - 1)
        self.rows = rest[:count]
        self.corners = (rest[count : 2 * count], rest[2 * count : 3 * count])
        self.even = is_even()

    def both(self, refs, index):
        if self.merged:
            return refs[0][index]
        upper = iota((TILE, LANES), 0) < TILE // 2
        return jnp.where(upper, refs[0][index], refs[1][index])

    def face(self, g, side, n):
        a, b, w = (ref[g, n] for ref in self.faces)
        b = jnp.where(self.closing, w, b)
        return jnp.where(self.even, a, b) if side else jnp.where(self.even, b, a)

    def pair(self, g, n):
        tile = self.both(self.rows, (g, n))
        return tile, pltpu.roll(tile, TILE // 2, 0)

    def corner(self, g, side):
        t, k = g // SHARE, g % SHARE
        a, b = (self.both(refs, (t,)) for refs in self.corners)
        tile = jnp.where(self.even, a, b) if side else jnp.where(self.even, b, a)
        return pltpu.roll(tile, TILE - 2 * k, 0) if k else tile


def slab_kernel(merged, own, face_a, face_b, face_w, *rest):
    slab = rest[-1]
    halo = Halo(merged, face_a, face_b, face_w, rest[:-1])
    fields, height = own.shape[:2]
    width = 2 * halo.rows[0].shape[1]
    slot, _ = group_and_slot()
    for g in range(fields):
        held = own[g]
        for side in range(2):
            for n in range(REACH):
                where = n + side * (width + REACH)
                moved = pltpu.roll(halo.face(g, side, n), slot_shift(where), 1)
                held = jnp.where(slot == where, moved, held)
        slab[g, 0:height] = held
        tiles = [(REACH - 1, halo.corner(g, 0)), (width + REACH, halo.corner(g, 1))]
        for n in range(width // 2):
            first, second = halo.pair(g, n)
            tiles += [(2 * n + REACH, first), (2 * n + 1 + REACH, second)]
        held = jnp.zeros((TILE, LANES), jnp.float32)
        for where, tile in tiles:
            held = jnp.where(slot == where, pltpu.roll(tile, slot_shift(where), 1), held)
        slab[g, height : height + TILE] = held


def relax(phases, solute, sums, solute_sum, theta, mobility):
    squares = phases[0] * phases[0]
    for phase in phases[1:]:
        squares = squares + phase * phase
    excess = (theta - coupling * solute) - squares
    fresh = []
    fresh_squares = None
    for g, phase in enumerate(phases):
        speed = step_rate * mobility[g]
        rate = speed * excess + (1.0 - 6.0 * stiffness * speed)
        new = phase * rate + (stiffness * speed) * sums[g]()
        fresh.append(new)
        fresh_squares = new * new if fresh_squares is None else fresh_squares + new * new
    kept = (1.0 - 6.0 * diffusion) - rejection * (fresh_squares - squares)
    fresh.append(solute * kept + diffusion * solute_sum())
    return fresh


def bulk_kernel(merged, state, zsum, mobility, shifts, face_a, face_b, face_w, *rest):
    done, lower, wide, first = rest[-10:-6]
    rims, sums, pending = rest[-6:-4], rest[-4:-2], rest[-2:]
    halo = Halo(merged, face_a, face_b, face_w, rest[:-10])
    fields, width, height, length = state.shape
    grains = fields - 1
    rows = height + TILE
    top = height + TILE
    span = float(length * lax.axis_size("gz"))
    base = lax.axis_index("gz") * length
    lane = iota((1, LANES), 1)
    slot_of, _ = group_and_slot()
    speeds = [mobility[g] for g in range(grains)]
    own = slice(TILE, TILE + height)

    def theta_of(shift):
        zpos = (base + lane - shift).astype(jnp.float32)
        return 1.0 - 2.0 * (zpos + 0.5) / span

    def put_rim(ref, g, x, tile):
        ref[g, x, 0:TILE] = tile
        ref[g, x, top : top + TILE] = tile

    for g in range(fields):
        for x in range(width):
            wide[g, x + REACH, own] = state[g, x]
        for side in range(2):
            for n in range(REACH):
                wide[g, n + side * (width + REACH), own] = halo.face(g, side, n)
        for n in range(width // 2):
            first_tile, second_tile = halo.pair(g, n)
            put_rim(wide, g, 2 * n + REACH, first_tile)
            put_rim(wide, g, 2 * n + 1 + REACH, second_tile)
        put_rim(wide, g, REACH - 1, halo.corner(g, 0))
        put_rim(wide, g, width + REACH, halo.corner(g, 1))
        for x in (0, width + 2 * REACH - 1):
            put_rim(wide, g, x, jnp.zeros((TILE, LANES), jnp.float32))

    mask_first = early_mask(shifts)
    theta_first = theta_of(shifts[0])

    def lateral(ref, g, x, with_rim):
        total = ref[g, x - 1, own] + ref[g, x + 1, own]
        total = total + ref[g, x, TILE - 1 : top - 1] + ref[g, x, TILE + 1 : top + 1]
        if not with_rim:
            return total
        rim = ref[g, x - 1, 0:TILE] + ref[g, x + 1, 0:TILE]
        rim = rim + ref[g, x, top - 1 : top - 1 + TILE] + ref[g, x, 1 : TILE + 1]
        return jnp.concatenate([total, rim], axis=0)

    def plane_first(x, zsum_own, zsum_rim):
        full = [wide[g, x, TILE : top + TILE] for g in range(fields)]
        parts = [
            lambda g=g: lateral(wide, g, x, True)
            + jnp.concatenate([zsum_own(g), zsum_rim(g)], axis=0)
            for g in range(fields)
        ]
        fresh = relax(full[:grains], full[grains], parts[:grains], parts[grains], theta_first, speeds)
        for g in range(fields):
            first[g, x - 1, own] = fresh[g][0:height]
            put_rim(first, g, x - 1, fresh[g][height:rows])

    def put_lower(slot, source):
        for g in range(fields):
            moved = pltpu.roll(source(g), slot, 1)
            lower[g] = jnp.where(slot_of * GROUP + REACH + 1 == slot, moved, lower[g])

    lower[...] = jnp.zeros_like(lower)
    for x in (1, width + REACH):
        plane_first(
            x,
            lambda g, x=x: along(wide[g, x, own], mask_first),
            lambda g, x=x: along(wide[g, x, 0:TILE], mask_first),
        )
    for g in range(fields):
        rims[0][g] = along(wide[g, REACH, 0:TILE], mask_first)

    def plane_of(x):
        return lambda g: jnp.concatenate([first[g, x, own], first[g, x, 0:TILE]], axis=0)

    @pl.loop(0, width // UNROLL)
    def _(block):
        for part in range(UNROLL):
            x = block * UNROLL + part
            now, after = rims[part % 2], rims[1 - part % 2]
            put_lower((x + 1) * GROUP + REACH + 1, plane_of(x))
            plane_first(x + REACH, lambda g: zsum[g, x], lambda g: now[g])
            for g in range(fields):
                after[g] = along(wide[g, x + REACH + 1, 0:TILE], mask_first)

    for x in (width, width + 1):
        put_lower((x + 1) * GROUP + REACH + 1, plane_of(x))

    theta_second = theta_of(REACH)
    mask_second = bottom_mask(lax.axis_index("gz") == 0)

    for g in range(fields):
        sums[0][g] = along(first[g, 1, own], mask_second)
        pending[1][g] = jnp.zeros((height, LANES), jnp.float32)

    def flush(held, x):
        for g in range(fields):
            done[g, x] = pltpu.roll(held[g], LANES - REACH, 1)

    @pl.loop(0, width // UNROLL)
    def _(block):
        for part in range(UNROLL):
            x = block * UNROLL + part
            now, after = part % 2, 1 - part % 2
            flush(pending[after], jnp.maximum(x - 1, 0))
            full = [first[g, x + 1, own] for g in range(fields)]
            parts = [
                lambda g=g: lateral(first, g, x + 1, False) + sums[now][g] for g in range(fields)
            ]
            fresh = relax(
                full[:grains], full[grains], parts[:grains], parts[grains], theta_second, speeds
            )
            for g in range(fields):
                pending[now][g] = fresh[g]
                sums[after][g] = along(first[g, x + 2, own], mask_second)

    flush(pending[1], width - 1)


def crown_kernel(done, slab, above, lower, marks, mobility, shifts, out, whole, sems):
    fields, rows = slab.shape[:2]
    grains = fields - 1
    width, height, length = done.shape[1:]
    span = float(length * lax.axis_size("gz"))
    base = lax.axis_index("gz") * length
    topmost = lax.axis_index("gz") == lax.axis_size("gz") - 1
    early = shifts[0] > 0
    _, place = group_and_slot()
    speeds = [mobility[g] for g in range(grains)]

    def entering(g):
        if g == grains:
            return jnp.full((rows, LANES), melt_solute, jnp.float32)
        return jnp.where(marks[...] == float(g), nucleus, 0.0)

    planted = (place >= REACH) & (place < 2 * REACH)
    zero = jnp.zeros((rows, LANES), jnp.float32)

    def theta_of(offset):
        zpos = (base + length + place - offset).astype(jnp.float32)
        return 1.0 - 2.0 * (zpos + 0.5) / span

    def around(p):
        total = pltpu.roll(p, GROUP, 1) + pltpu.roll(p, LANES - GROUP, 1)
        total = total + pltpu.roll(p, 1, 0) + pltpu.roll(p, rows - 1, 0)
        return total + pltpu.roll(p, 1, 1) + pltpu.roll(p, LANES - 1, 1)

    def advance(ps, theta):
        sums = [functools.partial(around, p) for p in ps]
        return relax(ps[:grains], ps[grains], sums[:grains], sums[grains], theta, speeds)

    before = []
    for g in range(fields):
        high = jnp.where(topmost, jnp.where(planted & early, entering(g), zero), above[g])
        before.append(jnp.where(place < REACH, slab[g], high))
    middle = advance(before, theta_of(REACH + shifts[0]))
    after = []
    for g in range(fields):
        value = middle[g]
        value = jnp.where(topmost & jnp.logical_not(early) & planted, entering(g), value)
        value = jnp.where(topmost & (place >= 2 * REACH), 0.0, value)
        after.append(jnp.where(place < REACH, lower[g], pltpu.roll(value, 1, 1)))
    final = advance(after, theta_of(REACH + 1 + REACH))

    top = iota((1, LANES), 1) >= LANES - 2 * REACH
    copies = []
    for g in range(fields):
        cut = final[g][0:height]
        for x in range(width):
            shift = (LANES - 2 * REACH - (x + REACH) * GROUP - 1) % LANES
            whole[g, x] = jnp.where(top, pltpu.roll(cut, shift, 1), done[g, x])
        copy = pltpu.make_async_copy(whole.at[g], out.at[g], sems.at[g])
        copy.start()
        copies.append(copy)
    for copy in copies:
        copy.wait()


def shape(*dims):
    return jax.ShapeDtypeStruct(dims, jnp.float32)


def call(kernel, outs, inputs, cost, specs=None, outs_specs=None, scratch=(), grant=24 << 20):
    return pl.pallas_call(
        kernel,
        out_shape=outs,
        in_specs=specs or [VMEM] * len(inputs),
        out_specs=outs_specs or jax.tree.map(lambda _: VMEM, outs),
        scratch_shapes=list(scratch),
        cost_estimate=pl.CostEstimate(flops=cost, bytes_accessed=cost, transcendentals=0),
        compiler_params=pltpu.CompilerParams(vmem_limit_bytes=grant),
    )(*inputs)


def shards(state, mobility, seeds, frame_shifts):
    fields, width, height, length = state.shape
    count_x, count_y, count_z = (lax.axis_size(a) for a in ("gx", "gy", "gz"))
    merged = count_y == 2
    rows = height + TILE
    groups = -(-fields // SHARE)
    whole = shape(fields, width, height, length)
    packed = shape(fields, rows, length)

    def partner(i, kind):
        return (i + 1) % count_x if (i % 2 == 0) == (kind == 0) else (i - 1) % count_x

    def swap(value, pairs):
        return lax.ppermute(value, "gx", pairs + [(j, i) for i, j in pairs])

    toward = [-1] if merged else [-1, 1]

    def diagonal(value, kind):
        return [
            lax.ppermute(
                value,
                ("gx", "gy"),
                [
                    (i * count_y + j, partner(i, kind) * count_y + (j + d) % count_y)
                    for i in range(count_x)
                    for j in range(count_y)
                ],
            )
            for d in toward
        ]

    block, face_a, face_b, edge, corner_a, corner_b = call(
        load_kernel,
        [
            whole,
            shape(fields, REACH, height, length),
            shape(fields, REACH, height, length),
            shape(fields, width // 2, TILE, length),
            shape(groups, TILE, length),
            shape(groups, TILE, length),
        ],
        [pltpu.with_memory_space_constraint(state, pltpu.HBM)],
        100000,
        specs=[pl.BlockSpec(memory_space=pltpu.HBM)],
        scratch=[pltpu.SemaphoreType.DMA((fields,))],
    )
    got_w = swap(face_b, [(0, count_x - 1)])
    near = [
        lax.ppermute(edge, "gy", [(j, (j + d) % count_y) for j in range(count_y)])
        for d in toward
    ]
    got_a = swap(face_a, [(i, i + 1) for i in range(0, count_x, 2)])
    got_b = swap(face_b, [(i, i + 1) for i in range(1, count_x - 1, 2)])
    far_b = diagonal(corner_b, 1)
    far_a = diagonal(corner_a, 0)
    zsum, own, marks = call(
        prepare_kernel,
        [whole, shape(fields, height, length), shape(rows, length)],
        [block, seeds, frame_shifts],
        5000000,
        specs=[VMEM, VMEM, SMEM],
    )
    halo = [got_a, got_b, got_w, *near, *far_a, *far_b]
    slab = call(functools.partial(slab_kernel, merged), packed, [own, *halo], 100000)
    above = lax.ppermute(slab, "gz", [(k, k - 1) for k in range(1, count_z)])
    done, lower = call(
        functools.partial(bulk_kernel, merged),
        [whole, packed],
        [block, zsum, mobility, frame_shifts, *halo],
        20000000,
        specs=[VMEM, VMEM, SMEM, SMEM] + [VMEM] * len(halo),
        scratch=[
            pltpu.VMEM((fields, width + 2 * REACH, rows + TILE, length), jnp.float32),
            pltpu.VMEM((fields, width + 2, rows + TILE, length), jnp.float32),
        ]
        + [pltpu.VMEM((fields, TILE, length), jnp.float32)] * 2
        + [pltpu.VMEM((fields, height, length), jnp.float32)] * 4,
    )
    return call(
        crown_kernel,
        whole,
        [done, slab, above, lower, marks, mobility, frame_shifts],
        100000,
        specs=[VMEM] * 5 + [SMEM, SMEM],
        outs_specs=pl.BlockSpec(memory_space=pltpu.HBM),
        scratch=[
            pltpu.VMEM((fields, width, height, length), jnp.float32),
            pltpu.SemaphoreType.DMA((fields,)),
        ],
    )


def solution(mesh):
    placed = (P(None, "gx", "gy", "gz"), P(), P(), P())
    return jax.shard_map(
        shards, mesh=mesh, in_specs=placed, out_specs=P(None, "gx", "gy", "gz"), check_vma=False
    )
```

```python
import functools

import jax
import jax.numpy as jnp
from jax import lax
from jax.experimental import pallas as pl
from jax.experimental.pallas import tpu as pltpu
from jax.sharding import PartitionSpec as P


step_rate = 0.1
stiffness = 0.7
coupling = 0.5
diffusion = 0.14
rejection = 0.5
nucleus = 0.3
melt_solute = 1.0

TILE = 8
LANES = 128
REACH = 2
GROUP = 6
SHARE = 4
UNROLL = 8

VMEM = pl.BlockSpec(memory_space=pltpu.VMEM)
SMEM = pl.BlockSpec(memory_space=pltpu.SMEM)


def iota(shape, axis):
    return lax.broadcasted_iota(jnp.int32, shape, axis)


def is_even():
    return lax.rem(lax.axis_index("gx"), 2) == 0


def group_and_slot(ahead=0):
    lane = iota((1, LANES), 1) + ahead
    slot = lax.shift_right_logical(lane * 43, 8)
    return slot, lane - slot * GROUP


def edge_tile(ref, g, x):
    rows = ref.shape[2]
    low = ref[g, x, 0:TILE]
    high = ref[g, x, rows - TILE : rows]
    return jnp.where(iota((TILE, LANES), 0) < TILE // 2, low, high)


def corner_rows(k):
    row = iota((TILE, LANES), 0)
    return (row == 2 * k) | (row == (2 * k + TILE - 1) % TILE)


def outer_face_kernel(state, face, sem):
    start = jnp.where(is_even(), 0, state.shape[1] - REACH)
    copy = pltpu.make_async_copy(state.at[:, pl.ds(start, REACH)], face, sem)
    copy.start()
    copy.wait()


def load_kernel(state, block, face_a, rows, corner_a, corner_b, sems):
    fields, width = state.shape[:2]
    even = is_even()
    last = width - REACH
    copies = [
        pltpu.make_async_copy(state.at[g], block.at[g], sems.at[g]) for g in range(fields)
    ]
    for copy in copies:
        copy.start()
    row = iota((TILE, LANES), 0)
    outer = (row < REACH) | (row >= TILE - REACH)
    near_a = jnp.where(even, width - 1, 0)
    near_b = jnp.where(even, 0, width - 1)
    held = [None, None]
    for g in range(fields):
        copies[g].wait()
        face_a[g] = block[g, pl.ds(jnp.where(even, last, 0), REACH)]
        for pair in range(width // 2):
            first = edge_tile(block, g, 2 * pair)
            second = edge_tile(block, g, 2 * pair + 1)
            rows[g, pair] = jnp.where(outer, first, pltpu.roll(second, TILE // 2, 0))
        t, k = g // SHARE, g % SHARE
        for n, (corner, x) in enumerate(((corner_a, near_a), (corner_b, near_b))):
            tile = edge_tile(block, g, x)
            if k:
                tile = jnp.where(corner_rows(k), pltpu.roll(tile, 2 * k, 0), held[n])
            held[n] = tile
            if k == SHARE - 1 or g == fields - 1:
                corner[t] = tile


def bottom_mask(active):
    return jnp.where((iota((1, LANES), 1) == REACH) & active, 0.0, 1.0)


def along(p, mask):
    return pltpu.roll(p, 1, 1) * mask + pltpu.roll(p, LANES - 1, 1)


def early_mask(shifts):
    return bottom_mask((lax.axis_index("gz") == 0) & (shifts[0] > 0))


def slot_shift(slot):
    return (slot * GROUP + REACH) % LANES


def prepare_kernel(state, seeds, shifts, zsum, own, marks):
    fields, width, height, _ = state.shape
    rows = height + TILE
    total_x, total_y = seeds.shape[2:]
    slot, place = group_and_slot()
    mask = early_mask(shifts)
    for g in range(fields):
        held = None
        for x in range(width):
            p = state[g, x]
            zsum[g, x] = along(p, mask)
            moved = pltpu.roll(p, slot_shift(x + REACH), 1)
            held = moved if held is None else jnp.where(slot == x + REACH, moved, held)
        own[g] = held

    step = jnp.where(shifts[0] > 0, 0, 1)
    row_y = iota((rows, total_y), 0)
    y = jnp.where(row_y >= height + TILE // 2, row_y - rows, row_y) + lax.axis_index("gy") * height
    y = jnp.where(y < 0, y + total_y, y)
    y = jnp.where(y >= total_y, y - total_y, y)
    pick_y = jnp.where(iota((rows, total_y), 1) == y, 1.0, 0.0)
    x = slot - REACH + lax.axis_index("gx") * width
    x = jnp.where(x < 0, x + total_x, x)
    x = jnp.where(x >= total_x, x - total_x, x)
    total = jnp.zeros((rows, LANES), jnp.float32)
    for k in range(REACH):
        chosen = seeds[step, k].astype(jnp.float32)
        across = lax.dot_general(
            pick_y, chosen, (((1,), (1,)), ((), ())), preferred_element_type=jnp.float32
        )
        pick_x = jnp.where((iota((total_x, LANES), 0) == x) & (place == REACH + k), 1.0, 0.0)
        total = total + jnp.dot(across, pick_x, preferred_element_type=jnp.float32)
    marks[...] = total


class Halo:
    def __init__(self, merged, face_a, face_b, rest):
        count = 1 if merged else 2
        self.merged = merged
        self.faces = (face_a, face_b)
        self.rows = rest[:count]
        self.corners = (rest[count : 2 * count], rest[2 * count : 3 * count])
        self.even = is_even()

    def both(self, refs, index):
        if self.merged:
            return refs[0][index]
        upper = iota((TILE, LANES), 0) < TILE // 2
        return jnp.where(upper, refs[0][index], refs[1][index])

    def face(self, g, side, n):
        a, b = (ref[g, n] for ref in self.faces)
        return jnp.where(self.even, a, b) if side else jnp.where(self.even, b, a)

    def pair(self, g, n):
        tile = self.both(self.rows, (g, n))
        return tile, pltpu.roll(tile, TILE // 2, 0)

    def corner(self, g, side):
        t, k = g // SHARE, g % SHARE
        a, b = (self.both(refs, (t,)) for refs in self.corners)
        tile = jnp.where(self.even, a, b) if side else jnp.where(self.even, b, a)
        return pltpu.roll(tile, TILE - 2 * k, 0) if k else tile


def slab_kernel(merged, own, face_a, face_b, *rest):
    slab = rest[-1]
    halo = Halo(merged, face_a, face_b, rest[:-1])
    fields, height = own.shape[:2]
    width = 2 * halo.rows[0].shape[1]
    slot, _ = group_and_slot()
    for g in range(fields):
        held = own[g]
        for side in range(2):
            for n in range(REACH):
                where = n + side * (width + REACH)
                moved = pltpu.roll(halo.face(g, side, n), slot_shift(where), 1)
                held = jnp.where(slot == where, moved, held)
        slab[g, 0:height] = held
        tiles = [(REACH - 1, halo.corner(g, 0)), (width + REACH, halo.corner(g, 1))]
        for n in range(width // 2):
            first, second = halo.pair(g, n)
            tiles += [(2 * n + REACH, first), (2 * n + 1 + REACH, second)]
        held = jnp.zeros((TILE, LANES), jnp.float32)
        for where, tile in tiles:
            held = jnp.where(slot == where, pltpu.roll(tile, slot_shift(where), 1), held)
        slab[g, height : height + TILE] = held


def relax(phases, solute, sums, solute_sum, theta, mobility):
    squares = phases[0] * phases[0]
    for phase in phases[1:]:
        squares = squares + phase * phase
    excess = (theta - coupling * solute) - squares
    fresh = []
    fresh_squares = None
    for g, phase in enumerate(phases):
        speed = step_rate * mobility[g]
        rate = speed * excess + (1.0 - 6.0 * stiffness * speed)
        new = phase * rate + (stiffness * speed) * sums[g]()
        fresh.append(new)
        fresh_squares = new * new if fresh_squares is None else fresh_squares + new * new
    kept = (1.0 - 6.0 * diffusion) - rejection * (fresh_squares - squares)
    fresh.append(solute * kept + diffusion * solute_sum())
    return fresh


def bulk_kernel(merged, state, zsum, mobility, shifts, face_a, face_b, *rest):
    done, lower, wide, first = rest[-10:-6]
    rims, sums, pending = rest[-6:-4], rest[-4:-2], rest[-2:]
    halo = Halo(merged, face_a, face_b, rest[:-10])
    fields, width, height, length = state.shape
    grains = fields - 1
    rows = height + TILE
    top = height + TILE
    span = float(length * lax.axis_size("gz"))
    base = lax.axis_index("gz") * length
    lane = iota((1, LANES), 1)
    slot_of, _ = group_and_slot(1)
    speeds = [mobility[g] for g in range(grains)]
    own = slice(TILE, TILE + height)

    def theta_of(shift):
        zpos = (base + lane - shift).astype(jnp.float32)
        return 1.0 - 2.0 * (zpos + 0.5) / span

    def put_rim(ref, g, x, tile):
        ref[g, x, 0:TILE] = tile
        ref[g, x, top : top + TILE] = tile

    for g in range(fields):
        for x in range(width):
            wide[g, x + REACH, own] = state[g, x]
        for side in range(2):
            for n in range(REACH):
                wide[g, n + side * (width + REACH), own] = halo.face(g, side, n)
        for n in range(width // 2):
            first_tile, second_tile = halo.pair(g, n)
            put_rim(wide, g, 2 * n + REACH, first_tile)
            put_rim(wide, g, 2 * n + 1 + REACH, second_tile)
        put_rim(wide, g, REACH - 1, halo.corner(g, 0))
        put_rim(wide, g, width + REACH, halo.corner(g, 1))
        for x in (0, width + 2 * REACH - 1):
            put_rim(wide, g, x, jnp.zeros((TILE, LANES), jnp.float32))

    mask_first = early_mask(shifts)
    theta_first = theta_of(shifts[0])

    def lateral(ref, g, x, with_rim):
        total = ref[g, x - 1, own] + ref[g, x + 1, own]
        total = total + ref[g, x, TILE - 1 : top - 1] + ref[g, x, TILE + 1 : top + 1]
        if not with_rim:
            return total
        rim = ref[g, x - 1, 0:TILE] + ref[g, x + 1, 0:TILE]
        rim = rim + ref[g, x, top - 1 : top - 1 + TILE] + ref[g, x, 1 : TILE + 1]
        return jnp.concatenate([total, rim], axis=0)

    def plane_first(x, zsum_own, zsum_rim):
        full = [wide[g, x, TILE : top + TILE] for g in range(fields)]
        parts = [
            lambda g=g: lateral(wide, g, x, True)
            + jnp.concatenate([zsum_own(g), zsum_rim(g)], axis=0)
            for g in range(fields)
        ]
        fresh = relax(full[:grains], full[grains], parts[:grains], parts[grains], theta_first, speeds)
        for g in range(fields):
            first[g, x - 1, own] = fresh[g][0:height]
            put_rim(first, g, x - 1, fresh[g][height:rows])

    def put_lower(slot, source):
        for g in range(fields):
            moved = pltpu.roll(source(g), slot, 1)
            lower[g] = jnp.where(slot_of * GROUP + REACH == slot, moved, lower[g])

    lower[...] = jnp.zeros_like(lower)
    for x in (1, width + REACH):
        plane_first(
            x,
            lambda g, x=x: along(wide[g, x, own], mask_first),
            lambda g, x=x: along(wide[g, x, 0:TILE], mask_first),
        )
    for g in range(fields):
        rims[0][g] = along(wide[g, REACH, 0:TILE], mask_first)

    def plane_of(x):
        return lambda g: jnp.concatenate([first[g, x, own], first[g, x, 0:TILE]], axis=0)

    @pl.loop(0, width // UNROLL)
    def _(block):
        for part in range(UNROLL):
            x = block * UNROLL + part
            now, after = rims[part % 2], rims[1 - part % 2]
            put_lower((x + 1) * GROUP + REACH, plane_of(x))
            plane_first(x + REACH, lambda g: zsum[g, x], lambda g: now[g])
            for g in range(fields):
                after[g] = along(wide[g, x + REACH + 1, 0:TILE], mask_first)

    for x in (width, width + 1):
        put_lower((x + 1) * GROUP + REACH, plane_of(x))

    theta_second = theta_of(REACH)
    mask_second = bottom_mask(lax.axis_index("gz") == 0)

    for g in range(fields):
        sums[0][g] = along(first[g, 1, own], mask_second)
        pending[1][g] = jnp.zeros((height, LANES), jnp.float32)

    def flush(held, x):
        for g in range(fields):
            done[g, x] = pltpu.roll(held[g], LANES - REACH, 1)

    @pl.loop(0, width // UNROLL)
    def _(block):
        for part in range(UNROLL):
            x = block * UNROLL + part
            now, after = part % 2, 1 - part % 2
            flush(pending[after], jnp.maximum(x - 1, 0))
            full = [first[g, x + 1, own] for g in range(fields)]
            parts = [
                lambda g=g: lateral(first, g, x + 1, False) + sums[now][g] for g in range(fields)
            ]
            fresh = relax(
                full[:grains], full[grains], parts[:grains], parts[grains], theta_second, speeds
            )
            for g in range(fields):
                pending[now][g] = fresh[g]
                sums[after][g] = along(first[g, x + 2, own], mask_second)

    flush(pending[1], width - 1)


def crown_kernel(done, slab, above, lower, marks, mobility, shifts, out, whole, sems):
    fields, rows = slab.shape[:2]
    grains = fields - 1
    width, height, length = done.shape[1:]
    span = float(length * lax.axis_size("gz"))
    base = lax.axis_index("gz") * length
    topmost = lax.axis_index("gz") == lax.axis_size("gz") - 1
    early = shifts[0] > 0
    _, place = group_and_slot()
    speeds = [mobility[g] for g in range(grains)]

    def entering(g):
        if g == grains:
            return jnp.full((rows, LANES), melt_solute, jnp.float32)
        return jnp.where(marks[...] == float(g), nucleus, 0.0)

    below = (place == 0) | (place == GROUP - 1)
    planted = (place >= REACH) & (place < 2 * REACH)
    zero = jnp.zeros((rows, LANES), jnp.float32)

    def theta_of(offset):
        zpos = (base + length + place - offset).astype(jnp.float32)
        return 1.0 - 2.0 * (zpos + 0.5) / span

    def around(p):
        total = pltpu.roll(p, GROUP, 1) + pltpu.roll(p, LANES - GROUP, 1)
        total = total + pltpu.roll(p, 1, 0) + pltpu.roll(p, rows - 1, 0)
        return total + pltpu.roll(p, 1, 1) + pltpu.roll(p, LANES - 1, 1)

    def advance(ps, theta):
        sums = [functools.partial(around, p) for p in ps]
        return relax(ps[:grains], ps[grains], sums[:grains], sums[grains], theta, speeds)

    before = []
    for g in range(fields):
        high = jnp.where(topmost, jnp.where(planted & early, entering(g), zero), above[g])
        before.append(jnp.where(place < REACH, slab[g], high))
    middle = advance(before, theta_of(REACH + shifts[0]))
    after = []
    for g in range(fields):
        value = middle[g]
        value = jnp.where(topmost & jnp.logical_not(early) & planted, entering(g), value)
        value = jnp.where(topmost & (place >= 2 * REACH), 0.0, value)
        after.append(jnp.where(below, lower[g], value))
    final = advance(after, theta_of(REACH + REACH))

    top = iota((1, LANES), 1) >= LANES - 2 * REACH
    copies = []
    for g in range(fields):
        cut = final[g][0:height]
        for x in range(width):
            shift = (LANES - 2 * REACH - (x + REACH) * GROUP) % LANES
            whole[g, x] = jnp.where(top, pltpu.roll(cut, shift, 1), done[g, x])
        copy = pltpu.make_async_copy(whole.at[g], out.at[g], sems.at[g])
        copy.start()
        copies.append(copy)
    for copy in copies:
        copy.wait()


def shape(*dims):
    return jax.ShapeDtypeStruct(dims, jnp.float32)


def call(kernel, outs, inputs, cost, specs=None, outs_specs=None, scratch=(), grant=24 << 20):
    return pl.pallas_call(
        kernel,
        out_shape=outs,
        in_specs=specs or [VMEM] * len(inputs),
        out_specs=outs_specs or jax.tree.map(lambda _: VMEM, outs),
        scratch_shapes=list(scratch),
        cost_estimate=pl.CostEstimate(flops=cost, bytes_accessed=cost, transcendentals=0),
        compiler_params=pltpu.CompilerParams(vmem_limit_bytes=grant),
    )(*inputs)


def shards(state, mobility, seeds, frame_shifts):
    fields, width, height, length = state.shape
    count_x, count_y, count_z = (lax.axis_size(a) for a in ("gx", "gy", "gz"))
    merged = count_y == 2
    rows = height + TILE
    groups = -(-fields // SHARE)
    whole = shape(fields, width, height, length)
    packed = shape(fields, rows, length)

    def partner(i, kind):
        return (i + 1) % count_x if (i % 2 == 0) == (kind == 0) else (i - 1) % count_x

    def swap(value, pairs):
        return lax.ppermute(value, "gx", pairs + [(j, i) for i, j in pairs])

    toward = [-1] if merged else [-1, 1]

    def diagonal(value, kind):
        return [
            lax.ppermute(
                value,
                ("gx", "gy"),
                [
                    (i * count_y + j, partner(i, kind) * count_y + (j + d) % count_y)
                    for i in range(count_x)
                    for j in range(count_y)
                ],
            )
            for d in toward
        ]

    held = pltpu.with_memory_space_constraint(state, pltpu.HBM)
    in_hbm = [pl.BlockSpec(memory_space=pltpu.HBM)]
    face = shape(fields, REACH, height, length)
    face_b = call(
        outer_face_kernel,
        face,
        [held],
        100000,
        specs=in_hbm,
        scratch=[pltpu.SemaphoreType.DMA(())],
    )
    got_b = swap(face_b, [(i, (i + 1) % count_x) for i in range(1, count_x, 2)])
    block, face_a, edge, corner_a, corner_b = call(
        load_kernel,
        [
            whole,
            face,
            shape(fields, width // 2, TILE, length),
            shape(groups, TILE, length),
            shape(groups, TILE, length),
        ],
        [held],
        100000,
        specs=in_hbm,
        scratch=[pltpu.SemaphoreType.DMA((fields,))],
    )
    near = [
        lax.ppermute(edge, "gy", [(j, (j + d) % count_y) for j in range(count_y)])
        for d in toward
    ]
    got_a = swap(face_a, [(i, i + 1) for i in range(0, count_x, 2)])
    far_b = diagonal(corner_b, 1)
    far_a = diagonal(corner_a, 0)
    zsum, own, marks = call(
        prepare_kernel,
        [whole, shape(fields, height, length), shape(rows, length)],
        [block, seeds, frame_shifts],
        5000000,
        specs=[VMEM, VMEM, SMEM],
    )
    halo = [got_a, got_b, *near, *far_a, *far_b]
    slab = call(functools.partial(slab_kernel, merged), packed, [own, *halo], 100000)
    above = lax.ppermute(slab, "gz", [(k, k - 1) for k in range(1, count_z)])
    done, lower = call(
        functools.partial(bulk_kernel, merged),
        [whole, packed],
        [block, zsum, mobility, frame_shifts, *halo],
        20000000,
        specs=[VMEM, VMEM, SMEM, SMEM] + [VMEM] * len(halo),
        scratch=[
            pltpu.VMEM((fields, width + 2 * REACH, rows + TILE, length), jnp.float32),
            pltpu.VMEM((fields, width + 2, rows + TILE, length), jnp.float32),
        ]
        + [pltpu.VMEM((fields, TILE, length), jnp.float32)] * 2
        + [pltpu.VMEM((fields, height, length), jnp.float32)] * 4,
    )
    return call(
        crown_kernel,
        whole,
        [done, slab, above, lower, marks, mobility, frame_shifts],
        100000,
        specs=[VMEM] * 5 + [SMEM, SMEM],
        outs_specs=pl.BlockSpec(memory_space=pltpu.HBM),
        scratch=[
            pltpu.VMEM((fields, width, height, length), jnp.float32),
            pltpu.SemaphoreType.DMA((fields,)),
        ],
    )


def solution(mesh):
    placed = (P(None, "gx", "gy", "gz"), P(), P(), P())
    return jax.shard_map(
        shards, mesh=mesh, in_specs=placed, out_specs=P(None, "gx", "gy", "gz"), check_vma=False
    )
```

```python
import functools
import math

import jax
import jax.numpy as jnp
from jax import lax
from jax.experimental import pallas as pl
from jax.experimental.pallas import tpu as pltpu
from jax.sharding import PartitionSpec as P


step_rate = 0.1
stiffness = 0.7
coupling = 0.5
diffusion = 0.14
rejection = 0.5
nucleus = 0.3
melt_solute = 1.0

TILE = 8
LANES = 128
REACH = 2
GROUP = 6
SHARE = 4
UNROLL = 16

VMEM = pl.BlockSpec(memory_space=pltpu.VMEM)
SMEM = pl.BlockSpec(memory_space=pltpu.SMEM)


def iota(shape, axis):
    return lax.broadcasted_iota(jnp.int32, shape, axis)


def is_even():
    return lax.rem(lax.axis_index("gx"), 2) == 0


def group_and_slot(ahead=0):
    lane = iota((1, LANES), 1) + ahead
    slot = lax.shift_right_logical(lane * 43, 8)
    return slot, lane - slot * GROUP


def edge_tile(ref, g, x):
    rows = ref.shape[2]
    low = ref[g, x, 0:TILE]
    high = ref[g, x, rows - TILE : rows]
    return jnp.where(iota((TILE, LANES), 0) < TILE // 2, low, high)


def corner_rows(k):
    row = iota((TILE, LANES), 0)
    return (row == 2 * k) | (row == (2 * k + TILE - 1) % TILE)


def outer_face_kernel(state, face, sem):
    start = jnp.where(is_even(), 0, state.shape[1] - REACH)
    copy = pltpu.make_async_copy(state.at[:, pl.ds(start, REACH)], face, sem)
    copy.start()
    copy.wait()


def rims_kernel(state, face_a, rows, corner_a, corner_b):
    fields, width = state.shape[:2]
    even = is_even()
    face_a[...] = state[:, pl.ds(jnp.where(even, width - REACH, 0), REACH)]
    row = iota((TILE, LANES), 0)
    outer = (row < REACH) | (row >= TILE - REACH)
    for g in range(fields):
        for pair in range(width // 2):
            first = edge_tile(state, g, 2 * pair)
            second = edge_tile(state, g, 2 * pair + 1)
            rows[g, pair] = jnp.where(outer, first, pltpu.roll(second, TILE // 2, 0))
    near_a = jnp.where(even, width - 1, 0)
    near_b = jnp.where(even, 0, width - 1)
    for corner, x in ((corner_a, near_a), (corner_b, near_b)):
        for t in range(corner.shape[0]):
            held = None
            for k in range(SHARE):
                g = t * SHARE + k
                if g < fields:
                    tile = edge_tile(state, g, x)
                    if k:
                        tile = jnp.where(corner_rows(k), pltpu.roll(tile, 2 * k, 0), held)
                    held = tile
            corner[t] = held


def bottom_mask(active):
    return jnp.where((iota((1, LANES), 1) == REACH) & active, 0.0, 1.0)


def along(p, mask):
    return pltpu.roll(p, 1, 1) * mask + pltpu.roll(p, LANES - 1, 1)


def early_mask(shifts):
    return bottom_mask((lax.axis_index("gz") == 0) & (shifts[0] > 0))


def slot_shift(slot):
    return (slot * GROUP + REACH) % LANES


def prepare_kernel(state, seeds, shifts, zsum, own, marks):
    fields, width, height, _ = state.shape
    rows = height + TILE
    total_x, total_y = seeds.shape[2:]
    slot, place = group_and_slot()
    mask = early_mask(shifts)
    for g in range(fields):
        held = None
        for x in range(width):
            p = state[g, x]
            zsum[g, x] = along(p, mask)
            moved = pltpu.roll(p, slot_shift(x + REACH), 1)
            held = moved if held is None else jnp.where(slot == x + REACH, moved, held)
        own[g] = held

    step = jnp.where(shifts[0] > 0, 0, 1)
    row_y = iota((rows, total_y), 0)
    y = jnp.where(row_y >= height + TILE // 2, row_y - rows, row_y) + lax.axis_index("gy") * height
    y = jnp.where(y < 0, y + total_y, y)
    y = jnp.where(y >= total_y, y - total_y, y)
    pick_y = jnp.where(iota((rows, total_y), 1) == y, 1.0, 0.0)
    x = slot - REACH + lax.axis_index("gx") * width
    x = jnp.where(x < 0, x + total_x, x)
    x = jnp.where(x >= total_x, x - total_x, x)
    total = jnp.zeros((rows, LANES), jnp.float32)
    for k in range(REACH):
        chosen = seeds[step, k].astype(jnp.float32)
        across = lax.dot_general(
            pick_y, chosen, (((1,), (1,)), ((), ())), preferred_element_type=jnp.float32
        )
        pick_x = jnp.where((iota((total_x, LANES), 0) == x) & (place == REACH + k), 1.0, 0.0)
        total = total + jnp.dot(across, pick_x, preferred_element_type=jnp.float32)
    marks[...] = total


class Halo:
    def __init__(self, merged, face_a, face_b, rest):
        count = 1 if merged else 2
        self.merged = merged
        self.faces = (face_a, face_b)
        self.rows = rest[:count]
        self.corners = (rest[count : 2 * count], rest[2 * count : 3 * count])
        self.even = is_even()

    def both(self, refs, index):
        if self.merged:
            return refs[0][index]
        upper = iota((TILE, LANES), 0) < TILE // 2
        return jnp.where(upper, refs[0][index], refs[1][index])

    def face(self, g, side, n):
        a, b = (ref[g, n] for ref in self.faces)
        return jnp.where(self.even, a, b) if side else jnp.where(self.even, b, a)

    def pair(self, g, n):
        tile = self.both(self.rows, (g, n))
        return tile, pltpu.roll(tile, TILE // 2, 0)

    def corner(self, g, side):
        t, k = g // SHARE, g % SHARE
        a, b = (self.both(refs, (t,)) for refs in self.corners)
        tile = jnp.where(self.even, a, b) if side else jnp.where(self.even, b, a)
        return pltpu.roll(tile, TILE - 2 * k, 0) if k else tile


def slab_kernel(merged, own, face_a, face_b, *rest):
    slab = rest[-1]
    halo = Halo(merged, face_a, face_b, rest[:-1])
    fields, height = own.shape[:2]
    width = 2 * halo.rows[0].shape[1]
    slot, _ = group_and_slot()
    for g in range(fields):
        held = own[g]
        for side in range(2):
            for n in range(REACH):
                where = n + side * (width + REACH)
                moved = pltpu.roll(halo.face(g, side, n), slot_shift(where), 1)
                held = jnp.where(slot == where, moved, held)
        slab[g, 0:height] = held
        tiles = [(REACH - 1, halo.corner(g, 0)), (width + REACH, halo.corner(g, 1))]
        for n in range(width // 2):
            first, second = halo.pair(g, n)
            tiles += [(2 * n + REACH, first), (2 * n + 1 + REACH, second)]
        held = jnp.zeros((TILE, LANES), jnp.float32)
        for where, tile in tiles:
            held = jnp.where(slot == where, pltpu.roll(tile, slot_shift(where), 1), held)
        slab[g, height : height + TILE] = held


def relax(phases, solute, sums, solute_sum, theta, mobility):
    squares = phases[0] * phases[0]
    for phase in phases[1:]:
        squares = squares + phase * phase
    excess = (theta - coupling * solute) - squares
    fresh = []
    fresh_squares = None
    for g, phase in enumerate(phases):
        speed = step_rate * mobility[g]
        rate = speed * excess + (1.0 - 6.0 * stiffness * speed)
        new = phase * rate + (stiffness * speed) * sums[g]()
        fresh.append(new)
        fresh_squares = new * new if fresh_squares is None else fresh_squares + new * new
    kept = (1.0 - 6.0 * diffusion) - rejection * (fresh_squares - squares)
    fresh.append(solute * kept + diffusion * solute_sum())
    return fresh


def bulk_kernel(merged, state, zsum, mobility, shifts, face_a, face_b, *rest):
    done, lower, wide, first = rest[-10:-6]
    rims, sums, pending = rest[-6:-4], rest[-4:-2], rest[-2:]
    halo = Halo(merged, face_a, face_b, rest[:-10])
    fields, width, height, length = state.shape
    grains = fields - 1
    rows = height + TILE
    top = height + TILE
    unroll = math.gcd(width, UNROLL)
    span = float(length * lax.axis_size("gz"))
    base = lax.axis_index("gz") * length
    lane = iota((1, LANES), 1)
    slot_of, _ = group_and_slot(1)
    speeds = [mobility[g] for g in range(grains)]
    own = slice(TILE, TILE + height)

    def theta_of(shift):
        zpos = (base + lane - shift).astype(jnp.float32)
        return 1.0 - 2.0 * (zpos + 0.5) / span

    def put_rim(ref, g, x, tile):
        ref[g, x, 0:TILE] = tile
        ref[g, x, top : top + TILE] = tile

    for g in range(fields):
        for x in range(width):
            wide[g, x + REACH, own] = state[g, x]
        for side in range(2):
            for n in range(REACH):
                wide[g, n + side * (width + REACH), own] = halo.face(g, side, n)
        for n in range(width // 2):
            first_tile, second_tile = halo.pair(g, n)
            put_rim(wide, g, 2 * n + REACH, first_tile)
            put_rim(wide, g, 2 * n + 1 + REACH, second_tile)
        put_rim(wide, g, REACH - 1, halo.corner(g, 0))
        put_rim(wide, g, width + REACH, halo.corner(g, 1))
        for x in (0, width + 2 * REACH - 1):
            put_rim(wide, g, x, jnp.zeros((TILE, LANES), jnp.float32))

    mask_first = early_mask(shifts)
    theta_first = theta_of(shifts[0])

    def lateral(ref, g, x, with_rim):
        total = ref[g, x - 1, own] + ref[g, x + 1, own]
        total = total + ref[g, x, TILE - 1 : top - 1] + ref[g, x, TILE + 1 : top + 1]
        if not with_rim:
            return total
        rim = ref[g, x - 1, 0:TILE] + ref[g, x + 1, 0:TILE]
        rim = rim + ref[g, x, top - 1 : top - 1 + TILE] + ref[g, x, 1 : TILE + 1]
        return jnp.concatenate([total, rim], axis=0)

    def plane_first(x, zsum_own, zsum_rim):
        full = [wide[g, x, TILE : top + TILE] for g in range(fields)]
        parts = [
            lambda g=g: lateral(wide, g, x, True)
            + jnp.concatenate([zsum_own(g), zsum_rim(g)], axis=0)
            for g in range(fields)
        ]
        fresh = relax(full[:grains], full[grains], parts[:grains], parts[grains], theta_first, speeds)
        for g in range(fields):
            first[g, x - 1, own] = fresh[g][0:height]
            put_rim(first, g, x - 1, fresh[g][height:rows])

    def put_lower(slot, source):
        for g in range(fields):
            moved = pltpu.roll(source(g), slot, 1)
            lower[g] = jnp.where(slot_of * GROUP + REACH == slot, moved, lower[g])

    lower[...] = jnp.zeros_like(lower)
    for x in (1, width + REACH):
        plane_first(
            x,
            lambda g, x=x: along(wide[g, x, own], mask_first),
            lambda g, x=x: along(wide[g, x, 0:TILE], mask_first),
        )
    for g in range(fields):
        rims[0][g] = along(wide[g, REACH, 0:TILE], mask_first)

    def plane_of(x):
        return lambda g: jnp.concatenate([first[g, x, own], first[g, x, 0:TILE]], axis=0)

    @pl.loop(0, width // unroll)
    def _(block):
        for part in range(unroll):
            x = block * unroll + part
            now, after = rims[part % 2], rims[1 - part % 2]
            put_lower((x + 1) * GROUP + REACH, plane_of(x))
            plane_first(x + REACH, lambda g: zsum[g, x], lambda g: now[g])
            for g in range(fields):
                after[g] = along(wide[g, x + REACH + 1, 0:TILE], mask_first)

    for x in (width, width + 1):
        put_lower((x + 1) * GROUP + REACH, plane_of(x))

    theta_second = theta_of(REACH)
    mask_second = bottom_mask(lax.axis_index("gz") == 0)

    for g in range(fields):
        sums[0][g] = along(first[g, 1, own], mask_second)
        pending[1][g] = jnp.zeros((height, LANES), jnp.float32)

    def flush(held, x):
        for g in range(fields):
            done[g, x] = pltpu.roll(held[g], LANES - REACH, 1)

    @pl.loop(0, width // unroll)
    def _(block):
        for part in range(unroll):
            x = block * unroll + part
            now, after = part % 2, 1 - part % 2
            flush(pending[after], jnp.maximum(x - 1, 0))
            full = [first[g, x + 1, own] for g in range(fields)]
            parts = [
                lambda g=g: lateral(first, g, x + 1, False) + sums[now][g] for g in range(fields)
            ]
            fresh = relax(
                full[:grains], full[grains], parts[:grains], parts[grains], theta_second, speeds
            )
            for g in range(fields):
                pending[now][g] = fresh[g]
                sums[after][g] = along(first[g, x + 2, own], mask_second)

    flush(pending[1], width - 1)


def crown_kernel(done, slab, above, lower, marks, mobility, shifts, out, whole, sems):
    fields, rows = slab.shape[:2]
    grains = fields - 1
    width, height, length = done.shape[1:]
    span = float(length * lax.axis_size("gz"))
    base = lax.axis_index("gz") * length
    topmost = lax.axis_index("gz") == lax.axis_size("gz") - 1
    early = shifts[0] > 0
    _, place = group_and_slot()
    speeds = [mobility[g] for g in range(grains)]

    def entering(g):
        if g == grains:
            return jnp.full((rows, LANES), melt_solute, jnp.float32)
        return jnp.where(marks[...] == float(g), nucleus, 0.0)

    below = (place == 0) | (place == GROUP - 1)
    planted = (place >= REACH) & (place < 2 * REACH)
    zero = jnp.zeros((rows, LANES), jnp.float32)

    def theta_of(offset):
        zpos = (base + length + place - offset).astype(jnp.float32)
        return 1.0 - 2.0 * (zpos + 0.5) / span

    def around(p):
        total = pltpu.roll(p, GROUP, 1) + pltpu.roll(p, LANES - GROUP, 1)
        total = total + pltpu.roll(p, 1, 0) + pltpu.roll(p, rows - 1, 0)
        return total + pltpu.roll(p, 1, 1) + pltpu.roll(p, LANES - 1, 1)

    def advance(ps, theta):
        sums = [functools.partial(around, p) for p in ps]
        return relax(ps[:grains], ps[grains], sums[:grains], sums[grains], theta, speeds)

    before = []
    for g in range(fields):
        high = jnp.where(topmost, jnp.where(planted & early, entering(g), zero), above[g])
        before.append(jnp.where(place < REACH, slab[g], high))
    middle = advance(before, theta_of(REACH + shifts[0]))
    after = []
    for g in range(fields):
        value = middle[g]
        value = jnp.where(topmost & jnp.logical_not(early) & planted, entering(g), value)
        value = jnp.where(topmost & (place >= 2 * REACH), 0.0, value)
        after.append(jnp.where(below, lower[g], value))
    final = advance(after, theta_of(REACH + REACH))

    top = iota((1, LANES), 1) >= LANES - 2 * REACH
    copies = []
    for g in range(fields):
        cut = final[g][0:height]
        for x in range(width):
            shift = (LANES - 2 * REACH - (x + REACH) * GROUP) % LANES
            whole[g, x] = jnp.where(top, pltpu.roll(cut, shift, 1), done[g, x])
        copy = pltpu.make_async_copy(whole.at[g], out.at[g], sems.at[g])
        copy.start()
        copies.append(copy)
    for copy in copies:
        copy.wait()


def shape(*dims):
    return jax.ShapeDtypeStruct(dims, jnp.float32)


def call(kernel, outs, inputs, cost, specs=None, outs_specs=None, scratch=(), grant=24 << 20):
    return pl.pallas_call(
        kernel,
        out_shape=outs,
        in_specs=specs or [VMEM] * len(inputs),
        out_specs=outs_specs or jax.tree.map(lambda _: VMEM, outs),
        scratch_shapes=list(scratch),
        cost_estimate=pl.CostEstimate(flops=cost, bytes_accessed=cost, transcendentals=0),
        compiler_params=pltpu.CompilerParams(vmem_limit_bytes=grant),
    )(*inputs)


def shards(state, mobility, seeds, frame_shifts):
    fields, width, height, length = state.shape
    count_x, count_y, count_z = (lax.axis_size(a) for a in ("gx", "gy", "gz"))
    merged = count_y == 2
    rows = height + TILE
    groups = -(-fields // SHARE)
    whole = shape(fields, width, height, length)
    packed = shape(fields, rows, length)

    def partner(i, kind):
        return (i + 1) % count_x if (i % 2 == 0) == (kind == 0) else (i - 1) % count_x

    def swap(value, pairs):
        return lax.ppermute(value, "gx", pairs + [(j, i) for i, j in pairs])

    toward = [-1] if merged else [-1, 1]

    def diagonal(value, kind):
        return [
            lax.ppermute(
                value,
                ("gx", "gy"),
                [
                    (i * count_y + j, partner(i, kind) * count_y + (j + d) % count_y)
                    for i in range(count_x)
                    for j in range(count_y)
                ],
            )
            for d in toward
        ]

    face = shape(fields, REACH, height, length)
    face_b = call(
        outer_face_kernel,
        face,
        [pltpu.with_memory_space_constraint(state, pltpu.HBM)],
        100000,
        specs=[pl.BlockSpec(memory_space=pltpu.HBM)],
        scratch=[pltpu.SemaphoreType.DMA(())],
    )
    got_b = swap(face_b, [(i, (i + 1) % count_x) for i in range(1, count_x, 2)])
    face_a, edge, corner_a, corner_b = call(
        rims_kernel,
        [
            face,
            shape(fields, width // 2, TILE, length),
            shape(groups, TILE, length),
            shape(groups, TILE, length),
        ],
        [state],
        100000,
    )
    near = [
        lax.ppermute(edge, "gy", [(j, (j + d) % count_y) for j in range(count_y)])
        for d in toward
    ]
    got_a = swap(face_a, [(i, i + 1) for i in range(0, count_x, 2)])
    far_b = diagonal(corner_b, 1)
    far_a = diagonal(corner_a, 0)
    zsum, own, marks = call(
        prepare_kernel,
        [whole, shape(fields, height, length), shape(rows, length)],
        [state, seeds, frame_shifts],
        5000000,
        specs=[VMEM, VMEM, SMEM],
    )
    halo = [got_a, got_b, *near, *far_a, *far_b]
    slab = call(functools.partial(slab_kernel, merged), packed, [own, *halo], 100000)
    above = lax.ppermute(slab, "gz", [(k, k - 1) for k in range(1, count_z)])
    done, lower = call(
        functools.partial(bulk_kernel, merged),
        [whole, packed],
        [state, zsum, mobility, frame_shifts, *halo],
        20000000,
        specs=[VMEM, VMEM, SMEM, SMEM] + [VMEM] * len(halo),
        scratch=[
            pltpu.VMEM((fields, width + 2 * REACH, rows + TILE, length), jnp.float32),
            pltpu.VMEM((fields, width + 2, rows + TILE, length), jnp.float32),
        ]
        + [pltpu.VMEM((fields, TILE, length), jnp.float32)] * 2
        + [pltpu.VMEM((fields, height, length), jnp.float32)] * 4,
    )
    return call(
        crown_kernel,
        whole,
        [done, slab, above, lower, marks, mobility, frame_shifts],
        100000,
        specs=[VMEM] * 5 + [SMEM, SMEM],
        outs_specs=pl.BlockSpec(memory_space=pltpu.HBM),
        scratch=[
            pltpu.VMEM((fields, width, height, length), jnp.float32),
            pltpu.SemaphoreType.DMA((fields,)),
        ],
    )


def solution(mesh):
    placed = (P(None, "gx", "gy", "gz"), P(), P(), P())
    return jax.shard_map(
        shards, mesh=mesh, in_specs=placed, out_specs=P(None, "gx", "gy", "gz"), check_vma=False
    )
```

```python
import functools
import math

import jax
import jax.numpy as jnp
from jax import lax
from jax.experimental import pallas as pl
from jax.experimental.pallas import tpu as pltpu
from jax.sharding import PartitionSpec as P


step_rate = 0.1
stiffness = 0.7
coupling = 0.5
diffusion = 0.14
rejection = 0.5
nucleus = 0.3
melt_solute = 1.0

TILE = 8
LANES = 128
REACH = 2
GROUP = 6
SHARE = 4
UNROLL = 16

VMEM = pl.BlockSpec(memory_space=pltpu.VMEM)
SMEM = pl.BlockSpec(memory_space=pltpu.SMEM)


def iota(shape, axis):
    return lax.broadcasted_iota(jnp.int32, shape, axis)


def is_even():
    return lax.rem(lax.axis_index("gx"), 2) == 0


def group_and_slot(ahead=0):
    lane = iota((1, LANES), 1) + ahead
    slot = lax.shift_right_logical(lane * 43, 8)
    return slot, lane - slot * GROUP


def edge_tile(ref, g, x):
    rows = ref.shape[2]
    low = ref[g, x, 0:TILE]
    high = ref[g, x, rows - TILE : rows]
    return jnp.where(iota((TILE, LANES), 0) < TILE // 2, low, high)


def corner_rows(k):
    row = iota((TILE, LANES), 0)
    return (row == 2 * k) | (row == (2 * k + TILE - 1) % TILE)


def outer_face_kernel(state, face, sem):
    start = jnp.where(is_even(), 0, state.shape[1] - REACH)
    copy = pltpu.make_async_copy(state.at[:, pl.ds(start, REACH)], face, sem)
    copy.start()
    copy.wait()


def rims_kernel(state, face_a, rows, corner_a, corner_b):
    fields, width = state.shape[:2]
    even = is_even()
    face_a[...] = state[:, pl.ds(jnp.where(even, width - REACH, 0), REACH)]
    row = iota((TILE, LANES), 0)
    outer = (row < REACH) | (row >= TILE - REACH)
    for g in range(fields):
        for pair in range(width // 2):
            first = edge_tile(state, g, 2 * pair)
            second = edge_tile(state, g, 2 * pair + 1)
            rows[g, pair] = jnp.where(outer, first, pltpu.roll(second, TILE // 2, 0))
    near_a = jnp.where(even, width - 1, 0)
    near_b = jnp.where(even, 0, width - 1)
    for corner, x in ((corner_a, near_a), (corner_b, near_b)):
        for t in range(corner.shape[0]):
            held = None
            for k in range(SHARE):
                g = t * SHARE + k
                if g < fields:
                    tile = edge_tile(state, g, x)
                    if k:
                        tile = jnp.where(corner_rows(k), pltpu.roll(tile, 2 * k, 0), held)
                    held = tile
            corner[t] = held


def bottom_mask(active):
    return jnp.where((iota((1, LANES), 1) == REACH) & active, 0.0, 1.0)


def along(p, mask):
    return pltpu.roll(p, 1, 1) * mask + pltpu.roll(p, LANES - 1, 1)


def heights(length, shift):
    span = float(length * lax.axis_size("gz"))
    zpos = lax.axis_index("gz") * length + iota((1, LANES), 1) - shift
    return 1.0 - 2.0 * (zpos.astype(jnp.float32) + 0.5) / span


def step_of(center, sums, theta, speeds):
    grains = len(center) - 1
    return relax(center[:grains], center[grains], sums[:grains], sums[grains], theta, speeds)


def early_mask(shifts):
    return bottom_mask((lax.axis_index("gz") == 0) & (shifts[0] > 0))


def slot_shift(slot):
    return (slot * GROUP + REACH) % LANES


def prepare_kernel(state, seeds, mobility, shifts, part, outer, own, below, marks, *sums):
    fields, width, height, length = state.shape
    rows = height + TILE
    total_x, total_y = seeds.shape[2:]
    slot, place = group_and_slot()
    ahead, _ = group_and_slot(1)
    mask = early_mask(shifts)
    theta = heights(length, shifts[0])
    speeds = [mobility[g] for g in range(fields - 1)]
    flat = state.reshape(fields * width * height, LANES)

    def lateral(g, x):
        start = (g * width + x) * height
        total = state[g, x - 1] + state[g, x + 1]
        return total + flat[start - 1 : start - 1 + height] + flat[start + 1 : start + 1 + height]

    for g in range(fields):
        sums[1][g] = along(state[g, 1], mask)
        outer[g, 0] = along(state[g, 0], mask)
        outer[g, 1] = along(state[g, width - 1], mask)
        below[g] = jnp.zeros((height, LANES), jnp.float32)
        own[g] = jnp.zeros((height, LANES), jnp.float32)
    for x in range(width):
        now, after = sums[x % 2], sums[1 - x % 2]
        for g in range(fields):
            moved = pltpu.roll(state[g, x], slot_shift(x + REACH), 1)
            own[g] = jnp.where(slot == x + REACH, moved, own[g])
            if 1 < x:
                moved = pltpu.roll(part[g, x - 2], slot_shift(x - 1 + REACH), 1)
                below[g] = jnp.where(ahead == x - 1 + REACH, moved, below[g])
        if 0 < x < width - 1:
            center = [state[g, x] for g in range(fields)]
            around = [lambda g=g: lateral(g, x) + now[g] for g in range(fields)]
            fresh = step_of(center, around, theta, speeds)
            for g in range(fields):
                part[g, x - 1] = fresh[g]
                if x + 1 < width - 1:
                    after[g] = along(state[g, x + 1], mask)

    step = jnp.where(shifts[0] > 0, 0, 1)
    row_y = iota((rows, total_y), 0)
    y = jnp.where(row_y >= height + TILE // 2, row_y - rows, row_y) + lax.axis_index("gy") * height
    y = jnp.where(y < 0, y + total_y, y)
    y = jnp.where(y >= total_y, y - total_y, y)
    pick_y = jnp.where(iota((rows, total_y), 1) == y, 1.0, 0.0)
    x = slot - REACH + lax.axis_index("gx") * width
    x = jnp.where(x < 0, x + total_x, x)
    x = jnp.where(x >= total_x, x - total_x, x)
    total = jnp.zeros((rows, LANES), jnp.float32)
    for k in range(REACH):
        chosen = seeds[step, k].astype(jnp.float32)
        across = lax.dot_general(
            pick_y, chosen, (((1,), (1,)), ((), ())), preferred_element_type=jnp.float32
        )
        pick_x = jnp.where((iota((total_x, LANES), 0) == x) & (place == REACH + k), 1.0, 0.0)
        total = total + jnp.dot(across, pick_x, preferred_element_type=jnp.float32)
    marks[...] = total


class Halo:
    def __init__(self, merged, face_a, face_b, rest):
        count = 1 if merged else 2
        self.merged = merged
        self.faces = (face_a, face_b)
        self.rows = rest[:count]
        self.corners = (rest[count : 2 * count], rest[2 * count : 3 * count])
        self.even = is_even()

    def both(self, refs, index):
        if self.merged:
            return refs[0][index]
        upper = iota((TILE, LANES), 0) < TILE // 2
        return jnp.where(upper, refs[0][index], refs[1][index])

    def face(self, g, side, n):
        a, b = (ref[g, n] for ref in self.faces)
        return jnp.where(self.even, a, b) if side else jnp.where(self.even, b, a)

    def pair(self, g, n):
        tile = self.both(self.rows, (g, n))
        return tile, pltpu.roll(tile, TILE // 2, 0)

    def corner(self, g, side):
        t, k = g // SHARE, g % SHARE
        a, b = (self.both(refs, (t,)) for refs in self.corners)
        tile = jnp.where(self.even, a, b) if side else jnp.where(self.even, b, a)
        return pltpu.roll(tile, TILE - 2 * k, 0) if k else tile


def slab_kernel(merged, own, face_a, face_b, *rest):
    slab = rest[-1]
    halo = Halo(merged, face_a, face_b, rest[:-1])
    fields, height = own.shape[:2]
    width = 2 * halo.rows[0].shape[1]
    slot, _ = group_and_slot()
    for g in range(fields):
        held = own[g]
        for side in range(2):
            for n in range(REACH):
                where = n + side * (width + REACH)
                moved = pltpu.roll(halo.face(g, side, n), slot_shift(where), 1)
                held = jnp.where(slot == where, moved, held)
        slab[g, 0:height] = held
        tiles = [(REACH - 1, halo.corner(g, 0)), (width + REACH, halo.corner(g, 1))]
        for n in range(width // 2):
            first, second = halo.pair(g, n)
            tiles += [(2 * n + REACH, first), (2 * n + 1 + REACH, second)]
        held = jnp.zeros((TILE, LANES), jnp.float32)
        for where, tile in tiles:
            held = jnp.where(slot == where, pltpu.roll(tile, slot_shift(where), 1), held)
        slab[g, height : height + TILE] = held


def relax(phases, solute, sums, solute_sum, theta, mobility):
    squares = phases[0] * phases[0]
    for phase in phases[1:]:
        squares = squares + phase * phase
    excess = (theta - coupling * solute) - squares
    fresh = []
    fresh_squares = None
    for g, phase in enumerate(phases):
        speed = step_rate * mobility[g]
        rate = speed * excess + (1.0 - 6.0 * stiffness * speed)
        new = phase * rate + (stiffness * speed) * sums[g]()
        fresh.append(new)
        fresh_squares = new * new if fresh_squares is None else fresh_squares + new * new
    kept = (1.0 - 6.0 * diffusion) - rejection * (fresh_squares - squares)
    fresh.append(solute * kept + diffusion * solute_sum())
    return fresh


def bulk_kernel(merged, state, part, outer, below, mobility, shifts, face_a, face_b, *rest):
    done, lower, first, edge, edge_sum, edge_new, beyond = rest[-11:-4]
    sums, pending = rest[-4:-2], rest[-2:]
    halo = Halo(merged, face_a, face_b, rest[:-11])
    fields, width, height, length = state.shape
    top = height + TILE
    unroll = math.gcd(width, UNROLL)
    chunk = next(c for c in (3, 2, 1) if (width + 2) % c == 0)
    ahead, _ = group_and_slot(1)
    speeds = [mobility[g] for g in range(fields - 1)]
    own = slice(TILE, TILE + height)
    row = iota((TILE, LANES), 0)
    half = row < TILE // 2
    mask_first = early_mask(shifts)
    theta_first = heights(length, shifts[0])

    def plane(g, x):
        if 0 <= x < width:
            return state[g, x]
        return halo.face(g, 0, x + REACH) if x < 0 else halo.face(g, 1, x - width)

    def fold(p, rim):
        low, high = p[0:TILE], p[height - TILE : height]
        upper = pltpu.roll(jnp.where(half, rim, high), REACH, 0)
        under = pltpu.roll(jnp.where(half, low, rim), TILE - REACH, 0)
        return jnp.where(half, upper, under)

    for g in range(fields):
        for n in range(width // 2):
            for x, rim in zip((2 * n, 2 * n + 1), halo.pair(g, n)):
                edge[g, x + REACH] = fold(state[g, x], rim)
        for side, x in ((0, -1), (1, width)):
            edge[g, x + REACH] = fold(plane(g, x), halo.corner(g, side))
            beyond[g, side] = along(plane(g, x), mask_first)
        for x in (-REACH, width + REACH - 1):
            p = plane(g, x)
            edge[g, x + REACH] = fold(p, p[0:TILE])
        for x in range(1, width - 1):
            first[g, x + 1, own] = part[g, x - 1]
    for g in range(fields):
        for i in range(width + 2):
            edge_sum[g, i] = along(edge[g, i + 1], mask_first)

    for x in (-1, 0, width - 1, width):
        zsums, side = (outer, int(x > 0)) if 0 <= x < width else (beyond, int(x > 0))

        def around(g):
            center = plane(g, x)
            total = plane(g, x - 1) + plane(g, x + 1) + zsums[g, side]
            return total + pltpu.roll(center, 1, 0) + pltpu.roll(center, height - 1, 0)

        center = [plane(g, x) for g in range(fields)]
        parts = [functools.partial(around, g) for g in range(fields)]
        fresh = step_of(center, parts, theta_first, speeds)
        for g in range(fields):
            first[g, x + 1, own] = fresh[g]

    for i in range(0, width + 2, chunk):

        def tiles(ref, g, start):
            return jnp.concatenate([ref[g, start + t] for t in range(chunk)], axis=0)

        def turned(g, shift):
            return jnp.concatenate(
                [pltpu.roll(edge[g, i + 1 + t], shift, 0) for t in range(chunk)], axis=0
            )

        def around(g):
            total = tiles(edge, g, i) + tiles(edge, g, i + 2) + tiles(edge_sum, g, i)
            return total + turned(g, 1) + turned(g, TILE - 1)

        center = [tiles(edge, g, i + 1) for g in range(fields)]
        parts = [functools.partial(around, g) for g in range(fields)]
        fresh = step_of(center, parts, theta_first, speeds)
        for g in range(fields):
            for t in range(chunk):
                tile = fresh[g][t * TILE : (t + 1) * TILE]
                edge_new[g, i + t] = tile
                first[g, i + t, top - 1 : top + 1] = tile[1:3]
                first[g, i + t, TILE - 1 : TILE + 1] = tile[5:7]

    for g in range(fields):
        held = below[g]
        for x in (-1, 0, width - 1, width):
            moved = pltpu.roll(first[g, x + 1, own], slot_shift(x + REACH), 1)
            held = jnp.where(ahead == x + REACH, moved, held)
        rim = jnp.zeros((TILE, LANES), jnp.float32)
        for i in range(width + 2):
            moved = pltpu.roll(edge_new[g, i], slot_shift(i + 1), 1)
            rim = jnp.where(ahead == i + 1, moved, rim)
        forward, back = pltpu.roll(rim, REACH, 0), pltpu.roll(rim, TILE - REACH, 0)
        lower[g, 0:height] = held
        lower[g, 0:TILE] = jnp.where(row == 0, forward, held[0:TILE])
        lower[g, height - TILE : height] = jnp.where(
            row == TILE - 1, back, held[height - TILE : height]
        )
        lower[g, height : height + TILE] = jnp.where(half, back, forward)

    def lateral(g, x):
        total = first[g, x - 1, own] + first[g, x + 1, own]
        return total + first[g, x, TILE - 1 : top - 1] + first[g, x, TILE + 1 : top + 1]

    theta_second = heights(length, REACH)
    mask_second = bottom_mask(lax.axis_index("gz") == 0)

    for g in range(fields):
        sums[0][g] = along(first[g, 1, own], mask_second)
        pending[1][g] = jnp.zeros((height, LANES), jnp.float32)

    def flush(held, x):
        for g in range(fields):
            done[g, x] = pltpu.roll(held[g], LANES - REACH, 1)

    @pl.loop(0, width // unroll)
    def _(block):
        for part in range(unroll):
            x = block * unroll + part
            now, after = part % 2, 1 - part % 2
            flush(pending[after], jnp.maximum(x - 1, 0))
            full = [first[g, x + 1, own] for g in range(fields)]
            parts = [lambda g=g: lateral(g, x + 1) + sums[now][g] for g in range(fields)]
            fresh = step_of(full, parts, theta_second, speeds)
            for g in range(fields):
                pending[now][g] = fresh[g]
                sums[after][g] = along(first[g, x + 2, own], mask_second)

    flush(pending[1], width - 1)


def crown_kernel(done, slab, above, lower, marks, mobility, shifts, out, whole, sems):
    fields, rows = slab.shape[:2]
    grains = fields - 1
    width, height, length = done.shape[1:]
    span = float(length * lax.axis_size("gz"))
    base = lax.axis_index("gz") * length
    topmost = lax.axis_index("gz") == lax.axis_size("gz") - 1
    early = shifts[0] > 0
    _, place = group_and_slot()
    speeds = [mobility[g] for g in range(grains)]

    def entering(g):
        if g == grains:
            return jnp.full((rows, LANES), melt_solute, jnp.float32)
        return jnp.where(marks[...] == float(g), nucleus, 0.0)

    below = (place == 0) | (place == GROUP - 1)
    planted = (place >= REACH) & (place < 2 * REACH)
    zero = jnp.zeros((rows, LANES), jnp.float32)

    def theta_of(offset):
        zpos = (base + length + place - offset).astype(jnp.float32)
        return 1.0 - 2.0 * (zpos + 0.5) / span

    def around(p):
        total = pltpu.roll(p, GROUP, 1) + pltpu.roll(p, LANES - GROUP, 1)
        total = total + pltpu.roll(p, 1, 0) + pltpu.roll(p, rows - 1, 0)
        return total + pltpu.roll(p, 1, 1) + pltpu.roll(p, LANES - 1, 1)

    def advance(ps, theta):
        sums = [functools.partial(around, p) for p in ps]
        return relax(ps[:grains], ps[grains], sums[:grains], sums[grains], theta, speeds)

    before = []
    for g in range(fields):
        high = jnp.where(topmost, jnp.where(planted & early, entering(g), zero), above[g])
        before.append(jnp.where(place < REACH, slab[g], high))
    middle = advance(before, theta_of(REACH + shifts[0]))
    after = []
    for g in range(fields):
        value = middle[g]
        value = jnp.where(topmost & jnp.logical_not(early) & planted, entering(g), value)
        value = jnp.where(topmost & (place >= 2 * REACH), 0.0, value)
        after.append(jnp.where(below, lower[g], value))
    final = advance(after, theta_of(REACH + REACH))

    top = iota((1, LANES), 1) >= LANES - 2 * REACH
    copies = []
    for g in range(fields):
        cut = final[g][0:height]
        for x in range(width):
            shift = (LANES - 2 * REACH - (x + REACH) * GROUP) % LANES
            whole[g, x] = jnp.where(top, pltpu.roll(cut, shift, 1), done[g, x])
        copy = pltpu.make_async_copy(whole.at[g], out.at[g], sems.at[g])
        copy.start()
        copies.append(copy)
    for copy in copies:
        copy.wait()


def shape(*dims):
    return jax.ShapeDtypeStruct(dims, jnp.float32)


def call(kernel, outs, inputs, cost, specs=None, outs_specs=None, scratch=(), grant=24 << 20):
    return pl.pallas_call(
        kernel,
        out_shape=outs,
        in_specs=specs or [VMEM] * len(inputs),
        out_specs=outs_specs or jax.tree.map(lambda _: VMEM, outs),
        scratch_shapes=list(scratch),
        cost_estimate=pl.CostEstimate(flops=cost, bytes_accessed=cost, transcendentals=0),
        compiler_params=pltpu.CompilerParams(vmem_limit_bytes=grant),
    )(*inputs)


def shards(state, mobility, seeds, frame_shifts):
    fields, width, height, length = state.shape
    count_x, count_y, count_z = (lax.axis_size(a) for a in ("gx", "gy", "gz"))
    merged = count_y == 2
    rows = height + TILE
    groups = -(-fields // SHARE)
    whole = shape(fields, width, height, length)
    packed = shape(fields, rows, length)

    def partner(i, kind):
        return (i + 1) % count_x if (i % 2 == 0) == (kind == 0) else (i - 1) % count_x

    def swap(value, pairs):
        return lax.ppermute(value, "gx", pairs + [(j, i) for i, j in pairs])

    toward = [-1] if merged else [-1, 1]

    def diagonal(value, kind):
        return [
            lax.ppermute(
                value,
                ("gx", "gy"),
                [
                    (i * count_y + j, partner(i, kind) * count_y + (j + d) % count_y)
                    for i in range(count_x)
                    for j in range(count_y)
                ],
            )
            for d in toward
        ]

    face = shape(fields, REACH, height, length)
    face_b = call(
        outer_face_kernel,
        face,
        [pltpu.with_memory_space_constraint(state, pltpu.HBM)],
        100000,
        specs=[pl.BlockSpec(memory_space=pltpu.HBM)],
        scratch=[pltpu.SemaphoreType.DMA(())],
    )
    got_b = swap(face_b, [(i, (i + 1) % count_x) for i in range(1, count_x, 2)])
    face_a, edge, corner_a, corner_b = call(
        rims_kernel,
        [
            face,
            shape(fields, width // 2, TILE, length),
            shape(groups, TILE, length),
            shape(groups, TILE, length),
        ],
        [state],
        100000,
    )
    near = [
        lax.ppermute(edge, "gy", [(j, (j + d) % count_y) for j in range(count_y)])
        for d in toward
    ]
    got_a = swap(face_a, [(i, i + 1) for i in range(0, count_x, 2)])
    far_b = diagonal(corner_b, 1)
    far_a = diagonal(corner_a, 0)
    sides = shape(fields, 2, height, length)
    flat = shape(fields, height, length)
    lines = pltpu.VMEM((fields, height, length), jnp.float32)
    part, outer, own, below, marks = call(
        prepare_kernel,
        [shape(fields, width - 2, height, length), sides, flat, flat, shape(rows, length)],
        [state, seeds, mobility, frame_shifts],
        5000000,
        specs=[VMEM, VMEM, SMEM, SMEM],
        scratch=[lines, lines],
    )
    halo = [got_a, got_b, *near, *far_a, *far_b]
    slab = call(functools.partial(slab_kernel, merged), packed, [own, *halo], 100000)
    above = lax.ppermute(slab, "gz", [(k, k - 1) for k in range(1, count_z)])
    done, lower = call(
        functools.partial(bulk_kernel, merged),
        [whole, packed],
        [state, part, outer, below, mobility, frame_shifts, *halo],
        20000000,
        specs=[VMEM] * 4 + [SMEM, SMEM] + [VMEM] * len(halo),
        scratch=[
            pltpu.VMEM((fields, width + 2, rows + TILE, length), jnp.float32),
            pltpu.VMEM((fields, width + 2 * REACH, TILE, length), jnp.float32),
            pltpu.VMEM((fields, width + 2, TILE, length), jnp.float32),
            pltpu.VMEM((fields, width + 2, TILE, length), jnp.float32),
            pltpu.VMEM((fields, 2, height, length), jnp.float32),
            lines,
            lines,
            lines,
            lines,
        ],
    )
    return call(
        crown_kernel,
        whole,
        [done, slab, above, lower, marks, mobility, frame_shifts],
        100000,
        specs=[VMEM] * 5 + [SMEM, SMEM],
        outs_specs=pl.BlockSpec(memory_space=pltpu.HBM),
        scratch=[
            pltpu.VMEM((fields, width, height, length), jnp.float32),
            pltpu.SemaphoreType.DMA((fields,)),
        ],
    )


def solution(mesh):
    placed = (P(None, "gx", "gy", "gz"), P(), P(), P())
    return jax.shard_map(
        shards, mesh=mesh, in_specs=placed, out_specs=P(None, "gx", "gy", "gz"), check_vma=False
    )
```

```python
import functools
import math

import jax
import jax.numpy as jnp
from jax import lax
from jax.experimental import pallas as pl
from jax.experimental.pallas import tpu as pltpu
from jax.sharding import PartitionSpec as P


step_rate = 0.1
stiffness = 0.7
coupling = 0.5
diffusion = 0.14
rejection = 0.5
nucleus = 0.3
melt_solute = 1.0

TILE = 8
LANES = 128
REACH = 2
GROUP = 6
SHARE = 4
TRIO = 3
UNROLL = 16

VMEM = pl.BlockSpec(memory_space=pltpu.VMEM)
SMEM = pl.BlockSpec(memory_space=pltpu.SMEM)


def iota(shape, axis):
    return lax.broadcasted_iota(jnp.int32, shape, axis)


def is_even():
    return lax.rem(lax.axis_index("gx"), 2) == 0


def group_and_slot(ahead=0):
    lane = iota((1, LANES), 1) + ahead
    slot = lax.shift_right_logical(lane * 43, 8)
    return slot, lane - slot * GROUP


def edge_tile(ref, g, x):
    rows = ref.shape[2]
    low = ref[g, x, 0:TILE]
    high = ref[g, x, rows - TILE : rows]
    return jnp.where(iota((TILE, LANES), 0) < TILE // 2, low, high)


def corner_rows(k):
    row = iota((TILE, LANES), 0)
    return (row == 2 * k) | (row == (2 * k + TILE - 1) % TILE)


def outer_face_kernel(state, face, sem):
    start = jnp.where(is_even(), 0, state.shape[1] - REACH)
    copy = pltpu.make_async_copy(state.at[:, pl.ds(start, REACH)], face, sem)
    copy.start()
    copy.wait()


def rims_kernel(state, face_a, rows, corner_a, corner_b):
    fields, width = state.shape[:2]
    even = is_even()
    face_a[...] = state[:, pl.ds(jnp.where(even, width - REACH, 0), REACH)]
    row = iota((TILE, LANES), 0)
    outer = (row < REACH) | (row >= TILE - REACH)
    for g in range(fields):
        for pair in range(width // 2):
            first = edge_tile(state, g, 2 * pair)
            second = edge_tile(state, g, 2 * pair + 1)
            rows[g, pair] = jnp.where(outer, first, pltpu.roll(second, TILE // 2, 0))
    near_a = jnp.where(even, width - 1, 0)
    near_b = jnp.where(even, 0, width - 1)
    for corner, x in ((corner_a, near_a), (corner_b, near_b)):
        for t in range(corner.shape[0]):
            held = None
            for k in range(SHARE):
                g = t * SHARE + k
                if g < fields:
                    tile = edge_tile(state, g, x)
                    if k:
                        tile = jnp.where(corner_rows(k), pltpu.roll(tile, 2 * k, 0), held)
                    held = tile
            corner[t] = held


def bottom_mask(active):
    return jnp.where((iota((1, LANES), 1) == REACH) & active, 0.0, 1.0)


def along(p, mask):
    return pltpu.roll(p, 1, 1) * mask + pltpu.roll(p, LANES - 1, 1)


def heights(length, place, shift):
    span = float(length * lax.axis_size("gz"))
    zpos = (lax.axis_index("gz") * length + place).astype(jnp.float32) - shift
    return 1.0 - 2.0 * (zpos + 0.5) / span


def unpack_table(table):
    grains = table.shape[0] - TILE
    return [table[g : g + 1] for g in range(grains)], table[grains : grains + 1]


def step_of(center, sums, theta, speeds):
    grains = len(center) - 1
    return relax(center[:grains], center[grains], sums[:grains], sums[grains], theta, speeds)


def early_mask(first_shift):
    return bottom_mask((lax.axis_index("gz") == 0) & (first_shift > 0))


def slot_shift(slot):
    return (slot * GROUP + REACH) % LANES


def prepare_kernel(state, seeds, mobility, shifts, part, outer, own, below, marks, table, *sums):
    fields, width, height, length = state.shape
    rows = height + TILE
    total_x, total_y = seeds.shape[2:]
    slot, place = group_and_slot()
    ahead, _ = group_and_slot(1)
    mask = early_mask(shifts[0])
    lane = iota((1, LANES), 1)
    moved_by = jnp.broadcast_to(shifts[0].astype(jnp.float32), (TILE, LANES))
    theta = heights(length, lane, moved_by[0:1])
    speeds = [step_rate * mobility[g] for g in range(fields - 1)]
    for g, speed in enumerate(speeds):
        table[g : g + 1] = jnp.broadcast_to(speed, (1, LANES))
    table[fields - 1 : fields - 1 + TILE] = moved_by
    flat = state.reshape(fields * width * height, LANES)

    def lateral(g, x):
        start = (g * width + x) * height
        total = state[g, x - 1] + state[g, x + 1]
        return total + flat[start - 1 : start - 1 + height] + flat[start + 1 : start + 1 + height]

    for g in range(fields):
        sums[1][g] = along(state[g, 1], mask)
        outer[g, 0] = along(state[g, 0], mask)
        outer[g, 1] = along(state[g, width - 1], mask)
        below[g] = jnp.zeros((height, LANES), jnp.float32)
        own[g] = jnp.zeros((height, LANES), jnp.float32)
    for x in range(width):
        now, after = sums[x % 2], sums[1 - x % 2]
        for g in range(fields):
            moved = pltpu.roll(state[g, x], slot_shift(x + REACH), 1)
            own[g] = jnp.where(slot == x + REACH, moved, own[g])
            if 1 < x:
                moved = pltpu.roll(part[g, x - 2], slot_shift(x - 1 + REACH), 1)
                below[g] = jnp.where(ahead == x - 1 + REACH, moved, below[g])
        if 0 < x < width - 1:
            center = [state[g, x] for g in range(fields)]
            around = [lambda g=g: lateral(g, x) + now[g] for g in range(fields)]
            fresh = step_of(center, around, theta, speeds)
            for g in range(fields):
                part[g, x - 1] = fresh[g]
                if x + 1 < width - 1:
                    after[g] = along(state[g, x + 1], mask)

    step = jnp.where(shifts[0] > 0, 0, 1)
    row_y = iota((rows, total_y), 0)
    y = jnp.where(row_y >= height + TILE // 2, row_y - rows, row_y) + lax.axis_index("gy") * height
    y = jnp.where(y < 0, y + total_y, y)
    y = jnp.where(y >= total_y, y - total_y, y)
    pick_y = jnp.where(iota((rows, total_y), 1) == y, 1.0, 0.0)
    x = slot - REACH + lax.axis_index("gx") * width
    x = jnp.where(x < 0, x + total_x, x)
    x = jnp.where(x >= total_x, x - total_x, x)
    total = jnp.zeros((rows, LANES), jnp.float32)
    for k in range(REACH):
        chosen = seeds[step, k].astype(jnp.float32)
        across = lax.dot_general(
            pick_y, chosen, (((1,), (1,)), ((), ())), preferred_element_type=jnp.float32
        )
        pick_x = jnp.where((iota((total_x, LANES), 0) == x) & (place == REACH + k), 1.0, 0.0)
        total = total + jnp.dot(across, pick_x, preferred_element_type=jnp.float32)
    marks[...] = total


class Halo:
    def __init__(self, merged, face_a, face_b, rest):
        count = 1 if merged else 2
        self.merged = merged
        self.faces = (face_a, face_b)
        self.rows = rest[:count]
        self.corners = (rest[count : 2 * count], rest[2 * count : 3 * count])
        self.even = is_even()

    def both(self, refs, index):
        if self.merged:
            return refs[0][index]
        upper = iota((TILE, LANES), 0) < TILE // 2
        return jnp.where(upper, refs[0][index], refs[1][index])

    def face(self, g, side, n):
        a, b = (ref[g, n] for ref in self.faces)
        return jnp.where(self.even, a, b) if side else jnp.where(self.even, b, a)

    def pair(self, g, n):
        tile = self.both(self.rows, (g, n))
        return tile, pltpu.roll(tile, TILE // 2, 0)

    def corner(self, g, side):
        t, k = g // SHARE, g % SHARE
        a, b = (self.both(refs, (t,)) for refs in self.corners)
        tile = jnp.where(self.even, a, b) if side else jnp.where(self.even, b, a)
        return pltpu.roll(tile, TILE - 2 * k, 0) if k else tile


def slab_kernel(merged, own, face_a, face_b, *rest):
    slab, message = rest[-2:]
    halo = Halo(merged, face_a, face_b, rest[:-2])
    fields, height = own.shape[:2]
    width = 2 * halo.rows[0].shape[1]
    slot, place = group_and_slot()
    row = iota((TILE, LANES), 0)
    for g in range(fields):
        held = own[g]
        for side in range(2):
            for n in range(REACH):
                where = n + side * (width + REACH)
                moved = pltpu.roll(halo.face(g, side, n), slot_shift(where), 1)
                held = jnp.where(slot == where, moved, held)
        slab[g, 0:height] = held
        tiles = [(REACH - 1, halo.corner(g, 0)), (width + REACH, halo.corner(g, 1))]
        for n in range(width // 2):
            first, second = halo.pair(g, n)
            tiles += [(2 * n + REACH, first), (2 * n + 1 + REACH, second)]
        held = jnp.zeros((TILE, LANES), jnp.float32)
        for where, tile in tiles:
            held = jnp.where(slot == where, pltpu.roll(tile, slot_shift(where), 1), held)
        slab[g, height : height + TILE] = held
    for t in range(message.shape[0]):
        a, b, c = (slab[TRIO * t + n] for n in range(TRIO))
        a = jnp.where(place < REACH, pltpu.roll(c, LANES - REACH, 1), a)
        b = jnp.where(place < REACH, pltpu.roll(c, LANES - 2 * REACH, 1), b)
        message[t, 0:height] = a[0:height]
        message[t, height : 2 * height] = b[0:height]
        message[t, 2 * height : 2 * height + TILE] = jnp.where(
            (row < REACH) | (row >= TILE - REACH),
            a[height:],
            pltpu.roll(b[height:], TILE // 2, 0),
        )


def relax(phases, solute, sums, solute_sum, theta, speeds):
    squares = phases[0] * phases[0]
    for phase in phases[1:]:
        squares = squares + phase * phase
    excess = (theta - coupling * solute) - squares
    fresh = []
    fresh_squares = None
    for g, phase in enumerate(phases):
        speed = speeds[g]
        rate = speed * excess + (1.0 - 6.0 * stiffness * speed)
        new = phase * rate + (stiffness * speed) * sums[g]()
        fresh.append(new)
        fresh_squares = new * new if fresh_squares is None else fresh_squares + new * new
    kept = (1.0 - 6.0 * diffusion) - rejection * (fresh_squares - squares)
    fresh.append(solute * kept + diffusion * solute_sum())
    return fresh


def bulk_kernel(merged, state, part, outer, below, table, face_a, face_b, *rest):
    done, lower, first, edge, edge_sum, edge_new, beyond = rest[-11:-4]
    sums, pending = rest[-4:-2], rest[-2:]
    halo = Halo(merged, face_a, face_b, rest[:-11])
    fields, width, height, length = state.shape
    top = height + TILE
    unroll = math.gcd(width, UNROLL)
    chunk = next(c for c in (3, 2, 1) if (width + 2) % c == 0)
    ahead, _ = group_and_slot(1)
    speeds, first_shift = unpack_table(table)
    lane = iota((1, LANES), 1)
    own = slice(TILE, TILE + height)
    row = iota((TILE, LANES), 0)
    half = row < TILE // 2
    mask_first = early_mask(first_shift)
    theta_first = heights(length, lane, first_shift)

    def plane(g, x):
        if 0 <= x < width:
            return state[g, x]
        return halo.face(g, 0, x + REACH) if x < 0 else halo.face(g, 1, x - width)

    def fold(p, rim):
        low, high = p[0:TILE], p[height - TILE : height]
        upper = pltpu.roll(jnp.where(half, rim, high), REACH, 0)
        under = pltpu.roll(jnp.where(half, low, rim), TILE - REACH, 0)
        return jnp.where(half, upper, under)

    for g in range(fields):
        for n in range(width // 2):
            for x, rim in zip((2 * n, 2 * n + 1), halo.pair(g, n)):
                edge[g, x + REACH] = fold(state[g, x], rim)
        for side, x in ((0, -1), (1, width)):
            edge[g, x + REACH] = fold(plane(g, x), halo.corner(g, side))
            beyond[g, side] = along(plane(g, x), mask_first)
        for x in (-REACH, width + REACH - 1):
            p = plane(g, x)
            edge[g, x + REACH] = fold(p, p[0:TILE])
        for x in range(1, width - 1):
            first[g, x + 1, own] = part[g, x - 1]
    for g in range(fields):
        for i in range(width + 2):
            edge_sum[g, i] = along(edge[g, i + 1], mask_first)

    for x in (-1, 0, width - 1, width):
        zsums, side = (outer, int(x > 0)) if 0 <= x < width else (beyond, int(x > 0))

        def around(g):
            center = plane(g, x)
            total = plane(g, x - 1) + plane(g, x + 1) + zsums[g, side]
            return total + pltpu.roll(center, 1, 0) + pltpu.roll(center, height - 1, 0)

        center = [plane(g, x) for g in range(fields)]
        parts = [functools.partial(around, g) for g in range(fields)]
        fresh = step_of(center, parts, theta_first, speeds)
        for g in range(fields):
            first[g, x + 1, own] = fresh[g]

    for i in range(0, width + 2, chunk):

        def tiles(ref, g, start):
            return jnp.concatenate([ref[g, start + t] for t in range(chunk)], axis=0)

        def turned(g, shift):
            return jnp.concatenate(
                [pltpu.roll(edge[g, i + 1 + t], shift, 0) for t in range(chunk)], axis=0
            )

        def around(g):
            total = tiles(edge, g, i) + tiles(edge, g, i + 2) + tiles(edge_sum, g, i)
            return total + turned(g, 1) + turned(g, TILE - 1)

        center = [tiles(edge, g, i + 1) for g in range(fields)]
        parts = [functools.partial(around, g) for g in range(fields)]
        fresh = step_of(center, parts, theta_first, speeds)
        for g in range(fields):
            for t in range(chunk):
                tile = fresh[g][t * TILE : (t + 1) * TILE]
                edge_new[g, i + t] = tile
                first[g, i + t, top - 1 : top + 1] = tile[1:3]
                first[g, i + t, TILE - 1 : TILE + 1] = tile[5:7]

    for g in range(fields):
        held = below[g]
        for x in (-1, 0, width - 1, width):
            moved = pltpu.roll(first[g, x + 1, own], slot_shift(x + REACH), 1)
            held = jnp.where(ahead == x + REACH, moved, held)
        rim = jnp.zeros((TILE, LANES), jnp.float32)
        for i in range(width + 2):
            moved = pltpu.roll(edge_new[g, i], slot_shift(i + 1), 1)
            rim = jnp.where(ahead == i + 1, moved, rim)
        forward, back = pltpu.roll(rim, REACH, 0), pltpu.roll(rim, TILE - REACH, 0)
        lower[g, 0:height] = held
        lower[g, 0:TILE] = jnp.where(row == 0, forward, held[0:TILE])
        lower[g, height - TILE : height] = jnp.where(
            row == TILE - 1, back, held[height - TILE : height]
        )
        lower[g, height : height + TILE] = jnp.where(half, back, forward)

    def lateral(g, x):
        total = first[g, x - 1, own] + first[g, x + 1, own]
        return total + first[g, x, TILE - 1 : top - 1] + first[g, x, TILE + 1 : top + 1]

    theta_second = heights(length, lane, float(REACH))
    mask_second = bottom_mask(lax.axis_index("gz") == 0)

    for g in range(fields):
        sums[0][g] = along(first[g, 1, own], mask_second)
        pending[1][g] = jnp.zeros((height, LANES), jnp.float32)

    def flush(held, x):
        for g in range(fields):
            done[g, x] = pltpu.roll(held[g], LANES - REACH, 1)

    @pl.loop(0, width // unroll)
    def _(block):
        for part in range(unroll):
            x = block * unroll + part
            now, after = part % 2, 1 - part % 2
            flush(pending[after], jnp.maximum(x - 1, 0))
            full = [first[g, x + 1, own] for g in range(fields)]
            parts = [lambda g=g: lateral(g, x + 1) + sums[now][g] for g in range(fields)]
            fresh = step_of(full, parts, theta_second, speeds)
            for g in range(fields):
                pending[now][g] = fresh[g]
                sums[after][g] = along(first[g, x + 2, own], mask_second)

    flush(pending[1], width - 1)


def crown_kernel(done, slab, above, lower, marks, table, out, whole, sems):
    fields, rows = slab.shape[:2]
    grains = fields - 1
    width, height, length = done.shape[1:]
    topmost = lax.axis_index("gz") == lax.axis_size("gz") - 1
    _, place = group_and_slot()
    speeds, first_shift = unpack_table(table)
    early = first_shift > 0

    def entering(g):
        if g == grains:
            return jnp.full((rows, LANES), melt_solute, jnp.float32)
        return jnp.where(marks[...] == float(g), nucleus, 0.0)

    below = (place == 0) | (place == GROUP - 1)
    planted = (place >= REACH) & (place < 2 * REACH)
    zero = jnp.zeros((rows, LANES), jnp.float32)

    def arrived(t):
        a, b = above[t, 0:height], above[t, height : 2 * height]
        rim = above[t, 2 * height : 2 * height + TILE]
        a = jnp.concatenate([a, rim], axis=0)
        b = jnp.concatenate([b, pltpu.roll(rim, TILE // 2, 0)], axis=0)
        c = jnp.where(
            place < 2 * REACH, pltpu.roll(a, REACH, 1), pltpu.roll(b, 2 * REACH, 1)
        )
        return a, b, c

    def around(p):
        total = pltpu.roll(p, GROUP, 1) + pltpu.roll(p, LANES - GROUP, 1)
        total = total + pltpu.roll(p, 1, 0) + pltpu.roll(p, rows - 1, 0)
        return total + pltpu.roll(p, 1, 1) + pltpu.roll(p, LANES - 1, 1)

    def advance(ps, theta):
        sums = [functools.partial(around, p) for p in ps]
        return relax(ps[:grains], ps[grains], sums[:grains], sums[grains], theta, speeds)

    before = []
    upper = [p for t in range(above.shape[0]) for p in arrived(t)]
    for g in range(fields):
        high = jnp.where(topmost, jnp.where(planted & early, entering(g), zero), upper[g])
        before.append(jnp.where(place < REACH, slab[g], high))
    middle = advance(before, heights(length, length - REACH + place, first_shift))
    after = []
    for g in range(fields):
        value = middle[g]
        value = jnp.where(topmost & jnp.logical_not(early) & planted, entering(g), value)
        value = jnp.where(topmost & (place >= 2 * REACH), 0.0, value)
        after.append(jnp.where(below, lower[g], value))
    final = advance(after, heights(length, length - REACH + place, float(REACH)))

    top = iota((1, LANES), 1) >= LANES - 2 * REACH
    copies = []
    for g in range(fields):
        cut = final[g][0:height]
        for x in range(width):
            shift = (LANES - 2 * REACH - (x + REACH) * GROUP) % LANES
            whole[g, x] = jnp.where(top, pltpu.roll(cut, shift, 1), done[g, x])
        copy = pltpu.make_async_copy(whole.at[g], out.at[g], sems.at[g])
        copy.start()
        copies.append(copy)
    for copy in copies:
        copy.wait()


def shape(*dims):
    return jax.ShapeDtypeStruct(dims, jnp.float32)


def call(kernel, outs, inputs, cost, specs=None, outs_specs=None, scratch=(), grant=24 << 20):
    return pl.pallas_call(
        kernel,
        out_shape=outs,
        in_specs=specs or [VMEM] * len(inputs),
        out_specs=outs_specs or jax.tree.map(lambda _: VMEM, outs),
        scratch_shapes=list(scratch),
        cost_estimate=pl.CostEstimate(flops=cost, bytes_accessed=cost, transcendentals=0),
        compiler_params=pltpu.CompilerParams(vmem_limit_bytes=grant),
    )(*inputs)


def shards(state, mobility, seeds, frame_shifts):
    fields, width, height, length = state.shape
    count_x, count_y, count_z = (lax.axis_size(a) for a in ("gx", "gy", "gz"))
    merged = count_y == 2
    rows = height + TILE
    groups = -(-fields // SHARE)
    whole = shape(fields, width, height, length)
    packed = shape(fields, rows, length)

    def partner(i, kind):
        return (i + 1) % count_x if (i % 2 == 0) == (kind == 0) else (i - 1) % count_x

    def swap(value, pairs):
        return lax.ppermute(value, "gx", pairs + [(j, i) for i, j in pairs])

    toward = [-1] if merged else [-1, 1]

    def diagonal(value, kind):
        return [
            lax.ppermute(
                value,
                ("gx", "gy"),
                [
                    (i * count_y + j, partner(i, kind) * count_y + (j + d) % count_y)
                    for i in range(count_x)
                    for j in range(count_y)
                ],
            )
            for d in toward
        ]

    face = shape(fields, REACH, height, length)
    face_b = call(
        outer_face_kernel,
        face,
        [pltpu.with_memory_space_constraint(state, pltpu.HBM)],
        100000,
        specs=[pl.BlockSpec(memory_space=pltpu.HBM)],
        scratch=[pltpu.SemaphoreType.DMA(())],
    )
    got_b = swap(face_b, [(i, (i + 1) % count_x) for i in range(1, count_x, 2)])
    face_a, edge, corner_a, corner_b = call(
        rims_kernel,
        [
            face,
            shape(fields, width // 2, TILE, length),
            shape(groups, TILE, length),
            shape(groups, TILE, length),
        ],
        [state],
        100000,
    )
    near = [
        lax.ppermute(edge, "gy", [(j, (j + d) % count_y) for j in range(count_y)])
        for d in toward
    ]
    got_a = swap(face_a, [(i, i + 1) for i in range(0, count_x, 2)])
    far_b = diagonal(corner_b, 1)
    far_a = diagonal(corner_a, 0)
    sides = shape(fields, 2, height, length)
    flat = shape(fields, height, length)
    lines = pltpu.VMEM((fields, height, length), jnp.float32)
    part, outer, own, below, marks, table = call(
        prepare_kernel,
        [
            shape(fields, width - 2, height, length),
            sides,
            flat,
            flat,
            shape(rows, length),
            shape(fields - 1 + TILE, length),
        ],
        [state, seeds, mobility, frame_shifts],
        5000000,
        specs=[VMEM, VMEM, SMEM, SMEM],
        scratch=[lines, lines],
    )
    halo = [got_a, got_b, *near, *far_a, *far_b]
    slab, message = call(
        functools.partial(slab_kernel, merged),
        [packed, shape(fields // TRIO, 2 * height + TILE, length)],
        [own, *halo],
        100000,
    )
    above = lax.ppermute(message, "gz", [(k, (k - 1) % count_z) for k in range(count_z)])
    done, lower = call(
        functools.partial(bulk_kernel, merged),
        [whole, packed],
        [state, part, outer, below, table, *halo],
        20000000,
        scratch=[
            pltpu.VMEM((fields, width + 2, rows + TILE, length), jnp.float32),
            pltpu.VMEM((fields, width + 2 * REACH, TILE, length), jnp.float32),
            pltpu.VMEM((fields, width + 2, TILE, length), jnp.float32),
            pltpu.VMEM((fields, width + 2, TILE, length), jnp.float32),
            pltpu.VMEM((fields, 2, height, length), jnp.float32),
            lines,
            lines,
            lines,
            lines,
        ],
    )
    return call(
        crown_kernel,
        whole,
        [done, slab, above, lower, marks, table],
        100000,
        outs_specs=pl.BlockSpec(memory_space=pltpu.HBM),
        scratch=[
            pltpu.VMEM((fields, width, height, length), jnp.float32),
            pltpu.SemaphoreType.DMA((fields,)),
        ],
    )


def solution(mesh):
    placed = (P(None, "gx", "gy", "gz"), P(), P(), P())
    return jax.shard_map(
        shards, mesh=mesh, in_specs=placed, out_specs=P(None, "gx", "gy", "gz"), check_vma=False
    )
```

```python
import functools
import math

import jax
import jax.numpy as jnp
from jax import lax
from jax.experimental import pallas as pl
from jax.experimental.pallas import tpu as pltpu
from jax.sharding import PartitionSpec as P


step_rate = 0.1
stiffness = 0.7
coupling = 0.5
diffusion = 0.14
rejection = 0.5
nucleus = 0.3
melt_solute = 1.0

TILE = 8
LANES = 128
REACH = 2
GROUP = 6
SHARE = 4
TRIO = 3
UNROLL = 16

VMEM = pl.BlockSpec(memory_space=pltpu.VMEM)
SMEM = pl.BlockSpec(memory_space=pltpu.SMEM)


def iota(shape, axis):
    return lax.broadcasted_iota(jnp.int32, shape, axis)


def is_even():
    return lax.rem(lax.axis_index("gx"), 2) == 0


def group_and_slot(ahead=0):
    lane = iota((1, LANES), 1) + ahead
    slot = lax.shift_right_logical(lane * 43, 8)
    return slot, lane - slot * GROUP


def edge_tile(ref, g, x):
    rows = ref.shape[2]
    low = ref[g, x, 0:TILE]
    high = ref[g, x, rows - TILE : rows]
    return jnp.where(iota((TILE, LANES), 0) < TILE // 2, low, high)


def corner_rows(k):
    row = iota((TILE, LANES), 0)
    return (row == 2 * k) | (row == (2 * k + TILE - 1) % TILE)


def outer_face_kernel(state, face, sem):
    start = jnp.where(is_even(), 0, state.shape[1] - REACH)
    copies = [
        pltpu.make_async_copy(state.at[g, pl.ds(start, REACH)], face.at[g], sem.at[g])
        for g in range(state.shape[0])
    ]
    for copy in copies:
        copy.start()
    for copy in copies:
        copy.wait()


def rims_kernel(state, face_a, rows, corner_a, corner_b):
    fields, width = state.shape[:2]
    even = is_even()
    face_a[...] = state[:, pl.ds(jnp.where(even, width - REACH, 0), REACH)]
    row = iota((TILE, LANES), 0)
    outer = (row < REACH) | (row >= TILE - REACH)
    for g in range(fields):
        for pair in range(width // 2):
            first = edge_tile(state, g, 2 * pair)
            second = edge_tile(state, g, 2 * pair + 1)
            rows[g, pair] = jnp.where(outer, first, pltpu.roll(second, TILE // 2, 0))
    near_a = jnp.where(even, width - 1, 0)
    near_b = jnp.where(even, 0, width - 1)
    for corner, x in ((corner_a, near_a), (corner_b, near_b)):
        for t in range(corner.shape[0]):
            held = None
            for k in range(SHARE):
                g = t * SHARE + k
                if g < fields:
                    tile = edge_tile(state, g, x)
                    if k:
                        tile = jnp.where(corner_rows(k), pltpu.roll(tile, 2 * k, 0), held)
                    held = tile
            corner[t] = held


def bottom_mask(active):
    return jnp.where((iota((1, LANES), 1) == REACH) & active, 0.0, 1.0)


def along(p, mask):
    return pltpu.roll(p, 1, 1) * mask + pltpu.roll(p, LANES - 1, 1)


def heights(length, place, shift):
    span = float(length * lax.axis_size("gz"))
    zpos = (lax.axis_index("gz") * length + place).astype(jnp.float32) - shift
    return 1.0 - 2.0 * (zpos + 0.5) / span


def unpack_table(table):
    grains = table.shape[0] - TILE
    return [table[g : g + 1] for g in range(grains)], table[grains : grains + 1]


def step_of(center, sums, theta, speeds):
    grains = len(center) - 1
    return relax(center[:grains], center[grains], sums[:grains], sums[grains], theta, speeds)


def early_mask(first_shift):
    return bottom_mask((lax.axis_index("gz") == 0) & (first_shift > 0))


def slot_shift(slot):
    return (slot * GROUP + REACH) % LANES


def prepare_kernel(state, seeds, mobility, shifts, part, outer, own, below, marks, table, *sums):
    fields, width, height, length = state.shape
    rows = height + TILE
    total_x, total_y = seeds.shape[2:]
    slot, place = group_and_slot()
    ahead, _ = group_and_slot(1)
    mask = early_mask(shifts[0])
    lane = iota((1, LANES), 1)
    moved_by = jnp.broadcast_to(shifts[0].astype(jnp.float32), (TILE, LANES))
    theta = heights(length, lane, moved_by[0:1])
    speeds = [step_rate * mobility[g] for g in range(fields - 1)]
    for g, speed in enumerate(speeds):
        table[g : g + 1] = jnp.broadcast_to(speed, (1, LANES))
    table[fields - 1 : fields - 1 + TILE] = moved_by
    flat = state.reshape(fields * width * height, LANES)

    def lateral(g, x):
        start = (g * width + x) * height
        total = state[g, x - 1] + state[g, x + 1]
        return total + flat[start - 1 : start - 1 + height] + flat[start + 1 : start + 1 + height]

    for g in range(fields):
        sums[1][g] = along(state[g, 1], mask)
        outer[g, 0] = along(state[g, 0], mask)
        outer[g, 1] = along(state[g, width - 1], mask)
        below[g] = jnp.zeros((height, LANES), jnp.float32)
        own[g] = jnp.zeros((height, LANES), jnp.float32)
    for x in range(width):
        now, after = sums[x % 2], sums[1 - x % 2]
        for g in range(fields):
            moved = pltpu.roll(state[g, x], slot_shift(x + REACH), 1)
            own[g] = jnp.where(slot == x + REACH, moved, own[g])
            if 1 < x:
                moved = pltpu.roll(part[g, x - 2], slot_shift(x - 1 + REACH), 1)
                below[g] = jnp.where(ahead == x - 1 + REACH, moved, below[g])
        if 0 < x < width - 1:
            center = [state[g, x] for g in range(fields)]
            around = [lambda g=g: lateral(g, x) + now[g] for g in range(fields)]
            fresh = step_of(center, around, theta, speeds)
            for g in range(fields):
                part[g, x - 1] = fresh[g]
                if x + 1 < width - 1:
                    after[g] = along(state[g, x + 1], mask)

    step = jnp.where(shifts[0] > 0, 0, 1)
    row_y = iota((rows, total_y), 0)
    y = jnp.where(row_y >= height + TILE // 2, row_y - rows, row_y) + lax.axis_index("gy") * height
    y = jnp.where(y < 0, y + total_y, y)
    y = jnp.where(y >= total_y, y - total_y, y)
    pick_y = jnp.where(iota((rows, total_y), 1) == y, 1.0, 0.0)
    x = slot - REACH + lax.axis_index("gx") * width
    x = jnp.where(x < 0, x + total_x, x)
    x = jnp.where(x >= total_x, x - total_x, x)
    total = jnp.zeros((rows, LANES), jnp.float32)
    for k in range(REACH):
        chosen = seeds[step, k].astype(jnp.float32)
        across = lax.dot_general(
            pick_y, chosen, (((1,), (1,)), ((), ())), preferred_element_type=jnp.float32
        )
        pick_x = jnp.where((iota((total_x, LANES), 0) == x) & (place == REACH + k), 1.0, 0.0)
        total = total + jnp.dot(across, pick_x, preferred_element_type=jnp.float32)
    marks[...] = total


class Halo:
    def __init__(self, merged, face_a, face_b, rest):
        count = 1 if merged else 2
        self.merged = merged
        self.faces = (face_a, face_b)
        self.rows = rest[:count]
        self.corners = (rest[count : 2 * count], rest[2 * count : 3 * count])
        self.even = is_even()

    def both(self, refs, index):
        if self.merged:
            return refs[0][index]
        upper = iota((TILE, LANES), 0) < TILE // 2
        return jnp.where(upper, refs[0][index], refs[1][index])

    def face(self, g, side, n):
        a, b = (ref[g, n] for ref in self.faces)
        return jnp.where(self.even, a, b) if side else jnp.where(self.even, b, a)

    def pair(self, g, n):
        tile = self.both(self.rows, (g, n))
        return tile, pltpu.roll(tile, TILE // 2, 0)

    def corner(self, g, side):
        t, k = g // SHARE, g % SHARE
        a, b = (self.both(refs, (t,)) for refs in self.corners)
        tile = jnp.where(self.even, a, b) if side else jnp.where(self.even, b, a)
        return pltpu.roll(tile, TILE - 2 * k, 0) if k else tile


def slab_kernel(merged, own, face_a, face_b, *rest):
    slab, message = rest[-2:]
    halo = Halo(merged, face_a, face_b, rest[:-2])
    fields, height = own.shape[:2]
    width = 2 * halo.rows[0].shape[1]
    slot, place = group_and_slot()
    row = iota((TILE, LANES), 0)
    for g in range(fields):
        held = own[g]
        for side in range(2):
            for n in range(REACH):
                where = n + side * (width + REACH)
                moved = pltpu.roll(halo.face(g, side, n), slot_shift(where), 1)
                held = jnp.where(slot == where, moved, held)
        slab[g, 0:height] = held
        tiles = [(REACH - 1, halo.corner(g, 0)), (width + REACH, halo.corner(g, 1))]
        for n in range(width // 2):
            first, second = halo.pair(g, n)
            tiles += [(2 * n + REACH, first), (2 * n + 1 + REACH, second)]
        held = jnp.zeros((TILE, LANES), jnp.float32)
        for where, tile in tiles:
            held = jnp.where(slot == where, pltpu.roll(tile, slot_shift(where), 1), held)
        slab[g, height : height + TILE] = held
    for t in range(message.shape[0]):
        a, b, c = (slab[TRIO * t + n] for n in range(TRIO))
        a = jnp.where(place < REACH, pltpu.roll(c, LANES - REACH, 1), a)
        b = jnp.where(place < REACH, pltpu.roll(c, LANES - 2 * REACH, 1), b)
        message[t, 0:height] = a[0:height]
        message[t, height : 2 * height] = b[0:height]
        message[t, 2 * height : 2 * height + TILE] = jnp.where(
            (row < REACH) | (row >= TILE - REACH),
            a[height:],
            pltpu.roll(b[height:], TILE // 2, 0),
        )


def relax(phases, solute, sums, solute_sum, theta, speeds):
    squares = phases[0] * phases[0]
    for phase in phases[1:]:
        squares = squares + phase * phase
    excess = (theta - coupling * solute) - squares
    fresh = []
    fresh_squares = None
    for g, phase in enumerate(phases):
        speed = speeds[g]
        rate = speed * excess + (1.0 - 6.0 * stiffness * speed)
        new = phase * rate + (stiffness * speed) * sums[g]()
        fresh.append(new)
        fresh_squares = new * new if fresh_squares is None else fresh_squares + new * new
    kept = (1.0 - 6.0 * diffusion) - rejection * (fresh_squares - squares)
    fresh.append(solute * kept + diffusion * solute_sum())
    return fresh


def bulk_kernel(merged, state, part, outer, below, table, face_a, face_b, *rest):
    done, lower, first, edge, edge_sum, edge_new, beyond = rest[-11:-4]
    sums, pending = rest[-4:-2], rest[-2:]
    halo = Halo(merged, face_a, face_b, rest[:-11])
    fields, width, height, length = state.shape
    top = height + TILE
    unroll = math.gcd(width, UNROLL)
    chunk = next(c for c in (3, 2, 1) if (width + 2) % c == 0)
    ahead, _ = group_and_slot(1)
    speeds, first_shift = unpack_table(table)
    lane = iota((1, LANES), 1)
    own = slice(TILE, TILE + height)
    row = iota((TILE, LANES), 0)
    half = row < TILE // 2
    mask_first = early_mask(first_shift)
    theta_first = heights(length, lane, first_shift)

    def plane(g, x):
        if 0 <= x < width:
            return state[g, x]
        return halo.face(g, 0, x + REACH) if x < 0 else halo.face(g, 1, x - width)

    def fold(p, rim):
        low, high = p[0:TILE], p[height - TILE : height]
        upper = pltpu.roll(jnp.where(half, rim, high), REACH, 0)
        under = pltpu.roll(jnp.where(half, low, rim), TILE - REACH, 0)
        return jnp.where(half, upper, under)

    for g in range(fields):
        for n in range(width // 2):
            for x, rim in zip((2 * n, 2 * n + 1), halo.pair(g, n)):
                edge[g, x + REACH] = fold(state[g, x], rim)
        for side, x in ((0, -1), (1, width)):
            edge[g, x + REACH] = fold(plane(g, x), halo.corner(g, side))
            beyond[g, side] = along(plane(g, x), mask_first)
        for x in (-REACH, width + REACH - 1):
            p = plane(g, x)
            edge[g, x + REACH] = fold(p, p[0:TILE])
        for x in range(1, width - 1):
            first[g, x + 1, own] = part[g, x - 1]
    for g in range(fields):
        for i in range(width + 2):
            edge_sum[g, i] = along(edge[g, i + 1], mask_first)

    for x in (-1, 0, width - 1, width):
        zsums, side = (outer, int(x > 0)) if 0 <= x < width else (beyond, int(x > 0))

        def around(g):
            center = plane(g, x)
            total = plane(g, x - 1) + plane(g, x + 1) + zsums[g, side]
            return total + pltpu.roll(center, 1, 0) + pltpu.roll(center, height - 1, 0)

        center = [plane(g, x) for g in range(fields)]
        parts = [functools.partial(around, g) for g in range(fields)]
        fresh = step_of(center, parts, theta_first, speeds)
        for g in range(fields):
            first[g, x + 1, own] = fresh[g]

    for i in range(0, width + 2, chunk):

        def tiles(ref, g, start):
            return jnp.concatenate([ref[g, start + t] for t in range(chunk)], axis=0)

        def turned(g, shift):
            return jnp.concatenate(
                [pltpu.roll(edge[g, i + 1 + t], shift, 0) for t in range(chunk)], axis=0
            )

        def around(g):
            total = tiles(edge, g, i) + tiles(edge, g, i + 2) + tiles(edge_sum, g, i)
            return total + turned(g, 1) + turned(g, TILE - 1)

        center = [tiles(edge, g, i + 1) for g in range(fields)]
        parts = [functools.partial(around, g) for g in range(fields)]
        fresh = step_of(center, parts, theta_first, speeds)
        for g in range(fields):
            for t in range(chunk):
                tile = fresh[g][t * TILE : (t + 1) * TILE]
                edge_new[g, i + t] = tile
                first[g, i + t, top - 1 : top + 1] = tile[1:3]
                first[g, i + t, TILE - 1 : TILE + 1] = tile[5:7]

    for g in range(fields):
        held = below[g]
        for x in (-1, 0, width - 1, width):
            moved = pltpu.roll(first[g, x + 1, own], slot_shift(x + REACH), 1)
            held = jnp.where(ahead == x + REACH, moved, held)
        rim = jnp.zeros((TILE, LANES), jnp.float32)
        for i in range(width + 2):
            moved = pltpu.roll(edge_new[g, i], slot_shift(i + 1), 1)
            rim = jnp.where(ahead == i + 1, moved, rim)
        forward, back = pltpu.roll(rim, REACH, 0), pltpu.roll(rim, TILE - REACH, 0)
        lower[g, 0:height] = held
        lower[g, 0:TILE] = jnp.where(row == 0, forward, held[0:TILE])
        lower[g, height - TILE : height] = jnp.where(
            row == TILE - 1, back, held[height - TILE : height]
        )
        lower[g, height : height + TILE] = jnp.where(half, back, forward)

    def lateral(g, x):
        total = first[g, x - 1, own] + first[g, x + 1, own]
        return total + first[g, x, TILE - 1 : top - 1] + first[g, x, TILE + 1 : top + 1]

    theta_second = heights(length, lane, float(REACH))
    mask_second = bottom_mask(lax.axis_index("gz") == 0)

    for g in range(fields):
        sums[0][g] = along(first[g, 1, own], mask_second)
        pending[1][g] = jnp.zeros((height, LANES), jnp.float32)

    def flush(held, x):
        for g in range(fields):
            done[g, x] = pltpu.roll(held[g], LANES - REACH, 1)

    @pl.loop(0, width // unroll)
    def _(block):
        for part in range(unroll):
            x = block * unroll + part
            now, after = part % 2, 1 - part % 2
            flush(pending[after], jnp.maximum(x - 1, 0))
            full = [first[g, x + 1, own] for g in range(fields)]
            parts = [lambda g=g: lateral(g, x + 1) + sums[now][g] for g in range(fields)]
            fresh = step_of(full, parts, theta_second, speeds)
            for g in range(fields):
                pending[now][g] = fresh[g]
                sums[after][g] = along(first[g, x + 2, own], mask_second)

    flush(pending[1], width - 1)


def crown_kernel(done, slab, above, lower, marks, table, out, whole, sems):
    fields, rows = slab.shape[:2]
    grains = fields - 1
    width, height, length = done.shape[1:]
    topmost = lax.axis_index("gz") == lax.axis_size("gz") - 1
    _, place = group_and_slot()
    speeds, first_shift = unpack_table(table)
    early = first_shift > 0

    def entering(g):
        if g == grains:
            return jnp.full((rows, LANES), melt_solute, jnp.float32)
        return jnp.where(marks[...] == float(g), nucleus, 0.0)

    below = (place == 0) | (place == GROUP - 1)
    planted = (place >= REACH) & (place < 2 * REACH)
    zero = jnp.zeros((rows, LANES), jnp.float32)

    def arrived(t):
        a, b = above[t, 0:height], above[t, height : 2 * height]
        rim = above[t, 2 * height : 2 * height + TILE]
        a = jnp.concatenate([a, rim], axis=0)
        b = jnp.concatenate([b, pltpu.roll(rim, TILE // 2, 0)], axis=0)
        c = jnp.where(
            place < 2 * REACH, pltpu.roll(a, REACH, 1), pltpu.roll(b, 2 * REACH, 1)
        )
        return a, b, c

    def around(p):
        total = pltpu.roll(p, GROUP, 1) + pltpu.roll(p, LANES - GROUP, 1)
        total = total + pltpu.roll(p, 1, 0) + pltpu.roll(p, rows - 1, 0)
        return total + pltpu.roll(p, 1, 1) + pltpu.roll(p, LANES - 1, 1)

    def advance(ps, theta):
        sums = [functools.partial(around, p) for p in ps]
        return relax(ps[:grains], ps[grains], sums[:grains], sums[grains], theta, speeds)

    before = []
    upper = [p for t in range(above.shape[0]) for p in arrived(t)]
    for g in range(fields):
        high = jnp.where(topmost, jnp.where(planted & early, entering(g), zero), upper[g])
        before.append(jnp.where(place < REACH, slab[g], high))
    middle = advance(before, heights(length, length - REACH + place, first_shift))
    after = []
    for g in range(fields):
        value = middle[g]
        value = jnp.where(topmost & jnp.logical_not(early) & planted, entering(g), value)
        value = jnp.where(topmost & (place >= 2 * REACH), 0.0, value)
        after.append(jnp.where(below, lower[g], value))
    final = advance(after, heights(length, length - REACH + place, float(REACH)))

    top = iota((1, LANES), 1) >= LANES - 2 * REACH
    copies = []
    for g in range(fields):
        cut = final[g][0:height]
        for x in range(width):
            shift = (LANES - 2 * REACH - (x + REACH) * GROUP) % LANES
            whole[g, x] = jnp.where(top, pltpu.roll(cut, shift, 1), done[g, x])
        copy = pltpu.make_async_copy(whole.at[g], out.at[g], sems.at[g])
        copy.start()
        copies.append(copy)
    for copy in copies:
        copy.wait()


def shape(*dims):
    return jax.ShapeDtypeStruct(dims, jnp.float32)


def call(kernel, outs, inputs, cost, specs=None, outs_specs=None, scratch=(), grant=24 << 20):
    return pl.pallas_call(
        kernel,
        out_shape=outs,
        in_specs=specs or [VMEM] * len(inputs),
        out_specs=outs_specs or jax.tree.map(lambda _: VMEM, outs),
        scratch_shapes=list(scratch),
        cost_estimate=pl.CostEstimate(flops=cost, bytes_accessed=cost, transcendentals=0),
        compiler_params=pltpu.CompilerParams(vmem_limit_bytes=grant),
    )(*inputs)


def shards(state, mobility, seeds, frame_shifts):
    fields, width, height, length = state.shape
    count_x, count_y, count_z = (lax.axis_size(a) for a in ("gx", "gy", "gz"))
    merged = count_y == 2
    rows = height + TILE
    groups = -(-fields // SHARE)
    whole = shape(fields, width, height, length)
    packed = shape(fields, rows, length)

    def partner(i, kind):
        return (i + 1) % count_x if (i % 2 == 0) == (kind == 0) else (i - 1) % count_x

    def swap(value, pairs):
        return lax.ppermute(value, "gx", pairs + [(j, i) for i, j in pairs])

    toward = [-1] if merged else [-1, 1]

    def diagonal(value, kind):
        return [
            lax.ppermute(
                value,
                ("gx", "gy"),
                [
                    (i * count_y + j, partner(i, kind) * count_y + (j + d) % count_y)
                    for i in range(count_x)
                    for j in range(count_y)
                ],
            )
            for d in toward
        ]

    face = shape(fields, REACH, height, length)
    face_b = call(
        outer_face_kernel,
        face,
        [pltpu.with_memory_space_constraint(state, pltpu.HBM)],
        100000,
        specs=[pl.BlockSpec(memory_space=pltpu.HBM)],
        scratch=[pltpu.SemaphoreType.DMA((fields,))],
    )
    got_b = swap(face_b, [(i, (i + 1) % count_x) for i in range(1, count_x, 2)])
    face_a, edge, corner_a, corner_b = call(
        rims_kernel,
        [
            face,
            shape(fields, width // 2, TILE, length),
            shape(groups, TILE, length),
            shape(groups, TILE, length),
        ],
        [state],
        100000,
    )
    near = [
        lax.ppermute(edge, "gy", [(j, (j + d) % count_y) for j in range(count_y)])
        for d in toward
    ]
    got_a = swap(face_a, [(i, i + 1) for i in range(0, count_x, 2)])
    far_b = diagonal(corner_b, 1)
    far_a = diagonal(corner_a, 0)
    sides = shape(fields, 2, height, length)
    flat = shape(fields, height, length)
    lines = pltpu.VMEM((fields, height, length), jnp.float32)
    part, outer, own, below, marks, table = call(
        prepare_kernel,
        [
            shape(fields, width - 2, height, length),
            sides,
            flat,
            flat,
            shape(rows, length),
            shape(fields - 1 + TILE, length),
        ],
        [state, seeds, mobility, frame_shifts],
        5000000,
        specs=[VMEM, VMEM, SMEM, SMEM],
        scratch=[lines, lines],
    )
    halo = [got_a, got_b, *near, *far_a, *far_b]
    slab, message = call(
        functools.partial(slab_kernel, merged),
        [packed, shape(fields // TRIO, 2 * height + TILE, length)],
        [own, *halo],
        100000,
    )
    above = lax.ppermute(message, "gz", [(k, (k - 1) % count_z) for k in range(count_z)])
    done, lower = call(
        functools.partial(bulk_kernel, merged),
        [whole, packed],
        [state, part, outer, below, table, *halo],
        20000000,
        scratch=[
            pltpu.VMEM((fields, width + 2, rows + TILE, length), jnp.float32),
            pltpu.VMEM((fields, width + 2 * REACH, TILE, length), jnp.float32),
            pltpu.VMEM((fields, width + 2, TILE, length), jnp.float32),
            pltpu.VMEM((fields, width + 2, TILE, length), jnp.float32),
            pltpu.VMEM((fields, 2, height, length), jnp.float32),
            lines,
            lines,
            lines,
            lines,
        ],
    )
    return call(
        crown_kernel,
        whole,
        [done, slab, above, lower, marks, table],
        100000,
        outs_specs=pl.BlockSpec(memory_space=pltpu.HBM),
        scratch=[
            pltpu.VMEM((fields, width, height, length), jnp.float32),
            pltpu.SemaphoreType.DMA((fields,)),
        ],
    )


def solution(mesh):
    placed = (P(None, "gx", "gy", "gz"), P(), P(), P())
    return jax.shard_map(
        shards, mesh=mesh, in_specs=placed, out_specs=P(None, "gx", "gy", "gz"), check_vma=False
    )
```
